32 devices in a mesh: group: 4 (over z), shard: 8 (over y, x, core).
Axes of the slice: x: 2, y: 2, z: 4, core: 2. Of those that a mesh axis runs over, the one named last changes fastest.
Arguments:
- query_ids: int32 [256, 32], P(('group', 'shard')), may hold values from 0 to 30719
- word_table: bfloat16 [30720, 768], P('shard'), may hold values from -6 to 6
- pos_table: bfloat16 [32, 768], replicated, may hold values from -6 to 6
- emb_gain: float32 [768], replicated, may hold values from 0.25 to 1.75
- emb_bias: float32 [768], replicated, may hold values from -3 to 3
- w_qkv: bfloat16 [768, 2304], replicated, may hold values from -0.21875 to 0.21875
- b_qkv: float32 [2304], replicated, may hold values from -3 to 3
- w_out: bfloat16 [768, 768], replicated, may hold values from -0.21875 to 0.21875
- ln1_gain: float32 [768], replicated, may hold values from 0.25 to 1.75
- ln1_bias: float32 [768], replicated, may hold values from -3 to 3
- w_up: bfloat16 [768, 3072], replicated, may hold values from -0.21875 to 0.21875
- b_up: float32 [3072], replicated, may hold values from -3 to 3
- w_down: bfloat16 [3072, 768], replicated, may hold values from -0.109375 to 0.109375
- ln2_gain: float32 [768], replicated, may hold values from 0.25 to 1.75
- ln2_bias: float32 [768], replicated, may hold values from -3 to 3
- w_proj: bfloat16 [768, 128], replicated, may hold values from -0.21875 to 0.21875
- centroids: bfloat16 [16384, 128], replicated, may hold values from -0.59765625 to 0.59765625
- bucket_weights: float32 [4], replicated, may hold values from -0.12 to 0.12
- cand_store: int32 [256, 16], P(('group', 'shard')), may hold values from 0 to 31, all different within a row; in each aligned block of 8 rows (0 to 7, 8 to 15, ...) at most 8 rows name the same one
- cand_local: int32 [256, 16, 10], P(('group', 'shard')), may hold values from 0 to 31
- cent_ids: int32 [1024, 128], P(('group', 'shard')), may hold values from 0 to 16383
- residual_words: int32 [1024, 32, 128], P(('group', 'shard')), may hold values from 0 to 255
- lengths: int32 [1024], P(('group', 'shard')), may hold values from 16 to 128
Outputs:
- scores: float32 [256, 16, 10], P(('group', 'shard'))
The draws below stay inside these ranges and needn't reach their ends.
Inputs may be any that keep to these rules, and one draw needn't show every extreme that they name: `cand_store`: each row names 16 different devices; among the rows of one device no device is named more than 8 times, and some device is named exactly 8 times. `residual_words`: each word holds 4 two-bit codes.
All inputs are finite; a program needn't handle non-finite values.
Results may differ from the reference program's by a relative error of at most 0.004.
Values may be sent and summed in bfloat16 or wider, within the bound.
No kernel may reach another device: no remote copies, remote signals or barrier semaphores. Data moves between devices by JAX's collectives and lax.ppermute only.
A program may use at most 128 MiB of HBM per device.

```python
import math
import jax
import jax.numpy as jnp
import numpy as np
from jax import lax

D = 768
HEADS = 12
FF = 3072
DIM = 128
VOCAB = 30720
CENT = 16384
NBUCKET = 4
QLEN = 32
PLEN = 128
KS = 16
M = 10
Q_DEV = 8
P_DEV = 32
QUERIES = 256
PASSAGES = 1024
CAP = 8
WORDS = 32
DEVICES = 32


def touch_ends(result, key, smallest, high):
    dims = result.shape
    spot = [jax.random.randint(jax.random.fold_in(key, axis), (), 0, dims[axis]) for axis in range(len(dims))]
    result = result.at[tuple(spot)].set(smallest)
    longest = dims.index(max(dims))
    spot[longest] = (spot[longest] + 1) % dims[longest]
    return result.at[tuple(spot)].set(high)


def levels(stream_key, shape, pieces, smallest, high):
    factor_of, own = 1.0, jax.random.fold_in(stream_key, 6)
    for dim, blocks in pieces:
        draws = jnp.exp(jax.random.uniform(jax.random.fold_in(own, dim), (blocks,), jnp.float32, smallest / len(pieces), high / len(pieces)))
        factor_of = factor_of * jnp.repeat(draws, shape[dim] // blocks).reshape([-1 if axis == dim else 1 for axis in range(len(shape))])
    return factor_of


def rank_table(amount, slope):
    loads = [(1 << 20) // math.isqrt(standing ** slope) + 1 for standing in range(1, amount + 1)]
    scale = 1 + sum(loads) // (1 << 30)
    return np.cumsum(np.array([max(1, weight // scale) for weight in loads]))


def ranked_ids(key, shape, amount, lean):
    listing = rank_table(amount, lean)
    ticket = jax.random.randint(jax.random.fold_in(key, 1), shape, 0, int(listing[amount - 1]))
    standing = jnp.searchsorted(jnp.asarray(listing, jnp.int32), ticket, side="right")
    return jax.random.permutation(jax.random.fold_in(key, 2), amount)[standing].astype(jnp.int32)


def routed_block(rng, own, number, rows, number_of, top, reach, lean):
    sequence = jax.random.permutation(rng, number_of)
    crowded, usual = load_shares(number_of, rows * top, reach, lean, True), load_shares(number_of, rows * top, reach, lean, False)
    places = jnp.arange(number_of)

    def named(tallies, rotation):
        used = int((tallies > 0).sum())
        fixed = max(1, used // 4)
        moved = fixed + (places - fixed + rotation * (used - fixed)) % max(1, number_of - fixed)
        return jnp.zeros((number_of,), jnp.int32).at[sequence[jnp.where(places < fixed, places, moved)]].set(jnp.asarray(tallies, jnp.int32))

    tallies = jnp.where(number % 4 == 0, named(crowded, number // 4), named(usual, number - number // 4 - 1))
    mixed = jax.random.permutation(jax.random.fold_in(own, 3), number_of)
    donor, taker = mixed[0:number_of // 2 * 2:2], mixed[1:number_of // 2 * 2:2]
    slack = jnp.minimum(tallies[donor] - 1, reach - tallies[taker]) // 2
    slack = jnp.where((donor == sequence[0]) | (taker == sequence[0]) | (tallies[taker] == 0), 0, jnp.maximum(slack, 0))
    moved = jax.random.randint(jax.random.fold_in(own, 4), (number_of // 2,), 0, 1 << 20) % (slack + 1)
    tallies = tallies.at[donor].add(-moved).at[taker].add(moved)
    members = jnp.searchsorted(jnp.cumsum(tallies), jnp.arange(rows * top), side="right").astype(jnp.int32)
    listing = members.reshape(top, rows).T
    listing = listing[jax.random.permutation(jax.random.fold_in(own, 1), rows)]
    rotation = jax.random.randint(jax.random.fold_in(own, 2), (rows, 1), 0, top)
    return jnp.take_along_axis(listing, (jnp.arange(top)[None, :] + rotation) % top, axis=1)


def load_shares(number_of, total, most, skew, full):
    weights = [(1 << 20) // math.isqrt(rank ** skew) + 1 for rank in range(1, number_of + 1)]
    largest = most if full else min(most, max(-(-total // number_of), total * weights[0] // sum(weights)))
    least = 1 if total - largest >= number_of - 1 else 0
    given, surplus = [largest] + [least] * (number_of - 1), total - largest - least * (number_of - 1)
    while surplus > 0:
        candidates = [i for i in range(1, number_of) if given[i] < largest] or [i for i in range(1, number_of) if given[i] < most]
        mass, left = sum([weights[i] for i in candidates]), surplus
        for i in candidates:
            addition = min(most - given[i], max(1, left * weights[i] // mass), surplus)
            given[i] = given[i] + addition
            surplus = surplus - addition
    return np.array(given)


def noise(own_key, extent, deviation, most, pieces=(), kind=jnp.bfloat16):
    loudness = levels(own_key, extent, pieces, -0.22, 0.18) if pieces else 1.0
    drawn = jax.random.normal(own_key, extent, jnp.float32) * deviation * loudness
    return jnp.minimum(jnp.maximum(drawn, -most), most).astype(kind)


def setup_inputs(seed: int = 0) -> dict:
    streams_of = jax.random.split(jax.random.key(seed), 24)
    query_ids = touch_ends(ranked_ids(streams_of[0], (QUERIES, QLEN), VOCAB, 2), jax.random.fold_in(streams_of[0], 3), 0, VOCAB - 1).astype(jnp.int32)
    word_table = noise(streams_of[1], (VOCAB, D), 1.0, 6.0, ((0, 8),))
    pos_table = noise(streams_of[2], (QLEN, D), 1.0, 6.0)
    emb_gain = jnp.clip(1.0 + 0.15 * jax.random.normal(streams_of[3], (D,), jnp.float32), 0.25, 1.75)
    emb_bias = noise(streams_of[4], (D,), 0.5, 3.0, (), jnp.float32)
    w_qkv = noise(streams_of[5], (D, 3 * D), D ** -0.5, 0.21875)
    b_qkv = noise(streams_of[6], (3 * D,), 0.5, 3.0, (), jnp.float32)
    w_out = noise(streams_of[7], (D, D), D ** -0.5, 0.21875)
    ln1_gain = jnp.clip(1.0 + 0.15 * jax.random.normal(streams_of[8], (D,), jnp.float32), 0.25, 1.75)
    ln1_bias = noise(streams_of[9], (D,), 0.5, 3.0, (), jnp.float32)
    w_up = noise(streams_of[10], (D, FF), D ** -0.5, 0.21875)
    b_up = noise(streams_of[11], (FF,), 0.5, 3.0, (), jnp.float32)
    w_down = noise(streams_of[12], (FF, D), FF ** -0.5, 0.109375)
    ln2_gain = jnp.clip(1.0 + 0.15 * jax.random.normal(streams_of[13], (D,), jnp.float32), 0.25, 1.75)
    ln2_bias = noise(streams_of[14], (D,), 0.5, 3.0, (), jnp.float32)
    w_proj = noise(streams_of[15], (D, DIM), D ** -0.5, 0.21875)
    centroids = noise(streams_of[16], (CENT, DIM), 0.09, 0.59765625)
    bucket_weights = jnp.clip(jax.random.uniform(streams_of[17], (NBUCKET,), jnp.float32, -0.12, 0.12), -0.12, 0.12)
    cand_store_keys = jax.random.split(jax.random.fold_in(streams_of[18], 1), QUERIES // Q_DEV)
    cand_store_turns = jax.random.permutation(jax.random.fold_in(streams_of[18], 3), QUERIES // Q_DEV)
    cand_store = jax.vmap(lambda own, number: routed_block(jax.random.fold_in(streams_of[18], 2), own, number, Q_DEV, DEVICES, KS, CAP, 2))(cand_store_keys, cand_store_turns).reshape((QUERIES, KS))
    cand_local = touch_ends(jax.random.randint(streams_of[19], (QUERIES, KS, M), 0, P_DEV), jax.random.fold_in(streams_of[19], 1), 0, P_DEV - 1).astype(jnp.int32)
    cent_ids = touch_ends(ranked_ids(streams_of[20], (PASSAGES, PLEN), CENT, 1), jax.random.fold_in(streams_of[20], 3), 0, CENT - 1).astype(jnp.int32)
    residual_words = touch_ends(jax.random.randint(streams_of[21], (PASSAGES, WORDS, PLEN), 0, 256), jax.random.fold_in(streams_of[21], 1), 0, 255).astype(jnp.int32)
    lengths = touch_ends(jax.random.randint(streams_of[22], (PASSAGES,), PLEN // 8, PLEN + 1), jax.random.fold_in(streams_of[22], 1), PLEN // 8, PLEN).astype(jnp.int32)
    return dict(query_ids=query_ids, word_table=word_table, pos_table=pos_table, emb_gain=emb_gain, emb_bias=emb_bias, w_qkv=w_qkv, b_qkv=b_qkv, w_out=w_out, ln1_gain=ln1_gain, ln1_bias=ln1_bias, w_up=w_up, b_up=b_up, w_down=w_down, ln2_gain=ln2_gain, ln2_bias=ln2_bias, w_proj=w_proj, centroids=centroids, bucket_weights=bucket_weights, cand_store=cand_store, cand_local=cand_local, cent_ids=cent_ids, residual_words=residual_words, lengths=lengths)


LN_EPS = 1e-12
UNIT_EPS = 1e-06

def layer_norm(values, gain, bias):
    center = values - lax.optimization_barrier(jnp.mean(values, -1, keepdims=True))
    spread = lax.optimization_barrier(jnp.mean(center * center, -1, keepdims=True))
    return center * lax.rsqrt(spread + LN_EPS) * gain + bias

def encode(query_ids, word_table, pos_table, emb_gain, emb_bias, w_qkv, b_qkv, w_out, ln1_gain, ln1_bias, w_up, b_up, w_down, ln2_gain, ln2_bias, w_proj):
    batch, qlen = query_ids.shape
    width = word_table.shape[1]
    head_size = width // HEADS
    embedded = word_table[query_ids].astype(jnp.float32) + pos_table.astype(jnp.float32)[None]
    hidden = layer_norm(embedded, emb_gain, emb_bias).reshape(batch * qlen, width)
    mixed = jnp.dot(hidden.astype(jnp.bfloat16), w_qkv, preferred_element_type=jnp.float32) + b_qkv
    mixed = mixed.astype(jnp.bfloat16).reshape(batch, qlen, 3, HEADS, head_size)
    query = mixed[:, :, 0].astype(jnp.float32)
    keys = mixed[:, :, 1].astype(jnp.float32)
    values = mixed[:, :, 2].astype(jnp.float32)
    logits = jnp.einsum('bqhd,bkhd->bhqk', query, keys) * head_size ** (-0.5)
    probs = jax.nn.softmax(logits, -1).astype(jnp.bfloat16)
    context = jnp.einsum('bhqk,bkhd->bqhd', probs.astype(jnp.float32), values)
    context = context.astype(jnp.bfloat16).reshape(batch * qlen, width)
    first = layer_norm(hidden + jnp.dot(context, w_out, preferred_element_type=jnp.float32), ln1_gain, ln1_bias)
    inner = jnp.dot(first.astype(jnp.bfloat16), w_up, preferred_element_type=jnp.float32) + b_up
    inner = jax.nn.gelu(inner, approximate=False).astype(jnp.bfloat16)
    second = layer_norm(first + jnp.dot(inner, w_down, preferred_element_type=jnp.float32), ln2_gain, ln2_bias)
    projected = jnp.dot(second.astype(jnp.bfloat16), w_proj, preferred_element_type=jnp.float32)
    unit = projected * lax.rsqrt(lax.optimization_barrier(jnp.sum(projected * projected, -1, keepdims=True)) + UNIT_EPS)
    return unit.astype(jnp.bfloat16).reshape(batch, qlen, -1)

def decompress(words, cent_rows, bucket_weights, centroids):
    shifts = 2 * jnp.arange(4, dtype=jnp.int32)
    codes = jnp.right_shift(words[..., :, None, :], shifts[:, None]) & 3
    codes = codes.reshape(words.shape[:-2] + (words.shape[-2] * 4, words.shape[-1]))
    residual = jnp.zeros(codes.shape, jnp.float32)
    for level in range(bucket_weights.shape[0]):
        residual = residual + jnp.where(codes == level, bucket_weights[level], jnp.float32(0.0))
    center = jnp.swapaxes(centroids[cent_rows].astype(jnp.float32), -1, -2)
    summed = center + residual
    unit = summed * lax.rsqrt(lax.optimization_barrier(jnp.sum(summed * summed, -2, keepdims=True)) + UNIT_EPS)
    return unit.astype(jnp.bfloat16)

def maxsim(query_rows, docs, lengths):
    sims = jnp.einsum('sqd,sdp->sqp', query_rows.astype(jnp.float32), docs.astype(jnp.float32))
    valid = jnp.arange(docs.shape[-1], dtype=jnp.int32)[None, None, :] < lengths[:, None, None]
    best = lax.optimization_barrier(jnp.max(jnp.where(valid, sims, -jnp.inf), -1))
    return lax.optimization_barrier(jnp.sum(best, -1))

def reference(query_ids, word_table, pos_table, emb_gain, emb_bias, w_qkv, b_qkv, w_out, ln1_gain, ln1_bias, w_up, b_up, w_down, ln2_gain, ln2_bias, w_proj, centroids, bucket_weights, cand_store, cand_local, cent_ids, residual_words, lengths):
    query_emb = encode(query_ids, word_table, pos_table, emb_gain, emb_bias, w_qkv, b_qkv, w_out, ln1_gain, ln1_bias, w_up, b_up, w_down, ln2_gain, ln2_bias, w_proj)

    def one_query(packed):
        emb, stores, picks = packed
        ident = (stores[:, None] * P_DEV + picks).reshape(-1).astype(jnp.int32)
        docs = decompress(residual_words[ident], cent_ids[ident], bucket_weights, centroids)
        repeated = jnp.broadcast_to(emb[None], (ident.shape[0],) + emb.shape)
        return maxsim(repeated, docs, lengths[ident]).reshape(picks.shape)
    return lax.map(one_query, (query_emb, cand_store, cand_local))
```

```python
import functools

import jax
import jax.numpy as jnp
from jax import lax
from jax.experimental import pallas as pl
from jax.experimental.pallas import tpu as pltpu
from jax.sharding import PartitionSpec as P

HEADS = 12
LN_EPS = 1e-12
UNIT_EPS = 1e-06
F32 = jnp.float32
BF16 = jnp.bfloat16
I32 = jnp.int32
VM = pl.BlockSpec(memory_space=pltpu.VMEM)
SM = pl.BlockSpec(memory_space=pltpu.SMEM)
ANY = pl.BlockSpec(memory_space=pl.ANY)
BOTH = ("group", "shard")


def dot(lhs, rhs):
    return jnp.dot(lhs, rhs, preferred_element_type=F32)


def dot_t(lhs, rhs):
    return lax.dot_general(lhs, rhs, (((1,), (1,)), ((), ())), preferred_element_type=F32)


def iota(shape, dim):
    return lax.broadcasted_iota(I32, shape, dim)


def three(values):
    high = values.astype(BF16)
    rest = values - high.astype(F32)
    mid = rest.astype(BF16)
    return high, mid, (rest - mid.astype(F32)).astype(BF16)


def layer_norm(values, gain, bias):
    center = values - jnp.mean(values, -1, keepdims=True)
    spread = jnp.mean(center * center, -1, keepdims=True)
    return center * lax.rsqrt(spread + LN_EPS) * gain + bias


def route_kernel(base_ref, ids_ref, list_ref, *, table_rows):
    n_dest, tokens = ids_ref.shape
    offset = ids_ref[...] - base_ref[0]
    inside = (offset >= 0) & (offset < table_rows)
    flags = inside.astype(F32)
    before = (iota((tokens, tokens), 0) < iota((tokens, tokens), 1)).astype(F32)
    rank = dot(flags.astype(BF16), before.astype(BF16)).astype(I32)
    rank = jnp.where(inside, rank, -1)
    kept = jnp.where(inside, offset, 0)
    high = jnp.right_shift(kept, 7).astype(F32).astype(BF16)
    low = (kept & 127).astype(F32).astype(BF16)
    places = iota((tokens, tokens), 0)
    for dest in range(n_dest):
        chosen = (places == rank[dest : dest + 1]).astype(F32).astype(BF16)
        pair = jnp.concatenate([high[dest : dest + 1], low[dest : dest + 1]], 0)
        moved = dot_t(pair, chosen).astype(I32)
        list_ref[dest : dest + 1, :] = moved[0:1] * 128 + moved[1:2]


def route(base, all_ids, table_rows):
    return pl.pallas_call(
        functools.partial(route_kernel, table_rows=table_rows),
        out_shape=jax.ShapeDtypeStruct(all_ids.shape, I32),
        in_specs=[SM, VM],
        out_specs=VM,
    )(base, all_ids)


def decode_kernel(levels_ref, lengths_ref, words_ref, center_ref, docs_ref):
    many, n_words, plen = words_ref.shape
    dim = center_ref.shape[1]
    each = dim // n_words
    spread = (iota((n_words, dim), 1) // each == iota((n_words, dim), 0)).astype(F32).astype(BF16)
    shifts = 2 * (iota((plen, dim), 1) % each)
    first = pl.program_id(0) * many
    for p in range(many):
        words = words_ref[p].astype(F32).T.astype(BF16)
        codes = jnp.right_shift(dot(words, spread).astype(I32), shifts) & 3
        residual = jnp.zeros(codes.shape, F32)
        for level in range(levels_ref.shape[0]):
            residual = residual + jnp.where(codes == level, levels_ref[level], 0.0)
        summed = center_ref[p * plen : (p + 1) * plen, :].astype(F32) + residual
        unit = summed * lax.rsqrt(jnp.sum(summed * summed, -1, keepdims=True) + UNIT_EPS)
        unit = jnp.where(iota(unit.shape, 0) < lengths_ref[first + p], unit, unit[0:1])
        docs_ref[p * plen : (p + 1) * plen, :] = unit.astype(BF16)


def decode(levels, lengths, words, center):
    passages, n_words, plen = words.shape
    dim = center.shape[1]
    many = 4
    return pl.pallas_call(
        decode_kernel,
        grid=(passages // many,),
        out_shape=jax.ShapeDtypeStruct(center.shape, BF16),
        in_specs=[
            SM,
            SM,
            pl.BlockSpec((many, n_words, plen), lambda i: (i, 0, 0)),
            pl.BlockSpec((many * plen, dim), lambda i: (i, 0)),
        ],
        out_specs=pl.BlockSpec((many * plen, dim), lambda i: (i, 0)),
    )(levels, lengths, words, center)


def encode_kernel(
    recv_ref,
    extra_ref,
    row_ref,
    column_ref,
    pos_ref,
    emb_gain,
    emb_bias,
    b_qkv,
    ln1_gain,
    ln1_bias,
    b_up,
    ln2_gain,
    ln2_bias,
    w_qkv_hbm,
    w_out_hbm,
    w_up_hbm,
    w_down_hbm,
    w_proj_hbm,
    out_ref,
    w_qkv,
    w_out,
    w_up,
    w_down,
    w_proj,
    mixed_ref,
    context_ref,
    sems,
    *,
    cap,
    table_rows,
):
    copies = []
    for k, (source, target) in enumerate(
        (
            (w_qkv_hbm, w_qkv),
            (w_out_hbm, w_out),
            (w_up_hbm, w_up),
            (w_down_hbm, w_down),
            (w_proj_hbm, w_proj),
        )
    ):
        copies.append(pltpu.make_async_copy(source, target, sems.at[k]))
        copies[-1].start()
    rows, width = extra_ref.shape
    qlen = pos_ref.shape[0]
    owner_row = row_ref[...] // table_rows
    owner_column = column_ref[...] // table_rows
    earlier = iota((rows, rows), 1) < iota((rows, rows), 0)
    same = ((owner_column == owner_row) & earlier).astype(F32)
    rank = jnp.sum(same, -1, keepdims=True).astype(I32)
    place = jnp.where(rank < cap, owner_column * cap + rank, -1)
    slots = recv_ref.shape[0]
    chosen = (iota((rows, slots), 1) == place).astype(F32).astype(BF16)
    own = dot(chosen, recv_ref[...]) + extra_ref[...].astype(F32)
    pos = pos_ref[...].astype(F32)
    embedded = own + jnp.concatenate([pos] * (rows // qlen), 0)
    hidden = layer_norm(embedded, emb_gain[...], emb_bias[...])
    copies[0].wait()
    mixed_ref[...] = (dot(hidden.astype(BF16), w_qkv[...]) + b_qkv[...]).astype(BF16)
    head = width // HEADS
    per = 128 // head
    scale = head ** (-0.5)
    outside = iota((rows, rows), 0) // qlen != iota((rows, rows), 1) // qlen
    bias = jnp.where(outside, -jnp.inf, 0.0)
    lane = iota((rows, 128), 1) // head
    for i in range(width // 128):
        query = mixed_ref[:, i * 128 : (i + 1) * 128]
        keys = mixed_ref[:, width + i * 128 : width + (i + 1) * 128]
        values = mixed_ref[:, 2 * width + i * 128 : 2 * width + (i + 1) * 128]
        context = jnp.zeros((rows, 128), F32)
        for h in range(per):
            mine = lane == h
            logits = dot_t(jnp.where(mine, query, jnp.zeros_like(query)), keys) * scale + bias
            powers = jnp.exp(logits - jnp.max(logits, -1, keepdims=True))
            probs = (powers / jnp.sum(powers, -1, keepdims=True)).astype(BF16)
            context = context + dot(probs, jnp.where(mine, values, jnp.zeros_like(values)))
        context_ref[:, i * 128 : (i + 1) * 128] = context.astype(BF16)
    copies[1].wait()
    first = layer_norm(hidden + dot(context_ref[...], w_out[...]), ln1_gain[...], ln1_bias[...])
    narrow = first.astype(BF16)
    hidden_units = w_up.shape[1]
    step = width
    copies[2].wait()
    copies[3].wait()
    total = jnp.zeros((rows, width), F32)
    for c in range(hidden_units // step):
        inner = dot(narrow, w_up[:, c * step : (c + 1) * step]) + b_up[:, c * step : (c + 1) * step]
        inner = 0.5 * inner * (1.0 + lax.erf(inner * (0.5**0.5)))
        total = total + dot(inner.astype(BF16), w_down[c * step : (c + 1) * step, :])
    second = layer_norm(first + total, ln2_gain[...], ln2_bias[...])
    copies[4].wait()
    projected = dot(second.astype(BF16), w_proj[...])
    unit = projected * lax.rsqrt(jnp.sum(projected * projected, -1, keepdims=True) + UNIT_EPS)
    out_ref[...] = unit.astype(BF16)


def encode(recv, extra, ids, pos, vectors, weights, cap, table_rows):
    rows = extra.shape[0]
    dim = weights[-1].shape[1]
    width = extra.shape[1]
    return pl.pallas_call(
        functools.partial(encode_kernel, cap=cap, table_rows=table_rows),
        out_shape=jax.ShapeDtypeStruct((rows, dim), BF16),
        in_specs=[VM] * (5 + len(vectors)) + [ANY] * len(weights),
        out_specs=VM,
        scratch_shapes=[pltpu.VMEM(w.shape, BF16) for w in weights]
        + [
            pltpu.VMEM((rows, 3 * width), BF16),
            pltpu.VMEM((rows, width), BF16),
            pltpu.SemaphoreType.DMA((len(weights),)),
        ],
        compiler_params=pltpu.CompilerParams(vmem_limit_bytes=48 * 1024 * 1024),
    )(
        recv,
        extra,
        ids.reshape(1, rows),
        ids.reshape(rows, 1),
        pos,
        *[v.reshape(1, -1) for v in vectors],
        *weights,
    )


def maxsim_kernel(source_ref, target_ref, query_ref, docs_ref, *rest, plen, qlen):
    out_ref, best_ref = rest[-2:]
    query = query_ref[0]
    rows = query.shape[0]
    tokens = docs_ref.shape[0]
    step = 2 * plen
    for k in range(tokens // step):
        sims = dot_t(docs_ref[k * step : (k + 1) * step, :], query)
        best_ref[2 * k : 2 * k + 2, :] = jnp.max(sims.reshape(2, plen, rows), 1)
    many = rows // qlen
    segment = (iota((16, rows), 1) // qlen == iota((16, rows), 0)).astype(F32).astype(BF16)
    high, mid, low = three(best_ref[...])
    total = dot_t(segment, high) + (dot_t(segment, mid) + dot_t(segment, low))
    out_ref[0] = total[:many]


def maxsim(query_blocks, source, target, docs, previous, devices, plen, qlen):
    rows, dim = query_blocks.shape[1:]
    tokens = docs.shape[0]
    passages = tokens // plen
    shape = (devices, rows // qlen, passages)
    extra = [] if previous is None else [previous]
    return pl.pallas_call(
        functools.partial(maxsim_kernel, plen=plen, qlen=qlen),
        grid_spec=pltpu.PrefetchScalarGridSpec(
            num_scalar_prefetch=2,
            grid=(source.shape[0],),
            in_specs=[
                pl.BlockSpec((1, rows, dim), lambda i, s, t: (s[i], 0, 0)),
                pl.BlockSpec((tokens, dim), lambda i, s, t: (0, 0)),
            ]
            + [ANY] * len(extra),
            out_specs=pl.BlockSpec((1,) + shape[1:], lambda i, s, t: (t[i], 0, 0)),
            scratch_shapes=[pltpu.VMEM((passages, rows), F32)],
        ),
        out_shape=jax.ShapeDtypeStruct(shape, F32),
        input_output_aliases={4: 0} if extra else {},
    )(source, target, query_blocks, docs, *extra)


def select_kernel(table_ref, store_ref, local_ref, out_ref, *, q_dev):
    pairs = store_ref.shape[0]
    rows, passages = table_ref.shape
    each = pairs // q_dev
    column = iota((pairs, rows), 1)
    wanted = store_ref[...] * q_dev + iota((pairs, 1), 0) // each
    chosen = (column == wanted).astype(F32).astype(BF16)
    high, mid, low = three(table_ref[...])
    own = dot(chosen, high) + (dot(chosen, mid) + dot(chosen, low))
    local = local_ref[...]
    result = jnp.zeros(local.shape, F32)
    for p in range(passages):
        result = jnp.where(local == p, own[:, p : p + 1], result)
    out_ref[...] = result


def select(table, store, local, q_dev):
    return pl.pallas_call(
        functools.partial(select_kernel, q_dev=q_dev),
        out_shape=jax.ShapeDtypeStruct(local.shape, F32),
        in_specs=[VM] * 3,
        out_specs=VM,
    )(table, store, local)


def on_device(
    query_ids,
    word_table,
    pos_table,
    emb_gain,
    emb_bias,
    w_qkv,
    b_qkv,
    w_out,
    ln1_gain,
    ln1_bias,
    w_up,
    b_up,
    w_down,
    ln2_gain,
    ln2_bias,
    w_proj,
    centroids,
    bucket_weights,
    cand_store,
    cand_local,
    cent_ids,
    residual_words,
    lengths,
):
    n_group = lax.axis_size("group")
    n_shard = lax.axis_size("shard")
    devices = n_group * n_shard
    group = lax.axis_index("group")
    shard = lax.axis_index("shard")
    q_dev, qlen = query_ids.shape
    table_rows, width = word_table.shape
    rows = q_dev * qlen
    plen = cent_ids.shape[1]
    many = cand_local.shape[2]
    cap = 3 * rows // n_shard

    ids = query_ids.reshape(rows)
    all_ids = lax.all_gather(ids, "shard", axis=0)
    asked = route(jnp.reshape(shard * table_rows, (1,)), all_ids, table_rows)

    def exchange(offsets):
        looked = word_table[offsets.reshape(-1)].reshape(n_shard, cap, width)
        return lax.all_to_all(looked, "shard", split_axis=0, concat_axis=0, tiled=True)

    recv = exchange(asked[:, :cap]).reshape(n_shard * cap, width)

    owners = all_ids // table_rows
    loads = jnp.sum((owners[..., None] == jnp.arange(n_shard)).astype(I32), 1)
    rounds = (jnp.max(loads) + cap - 1) // cap
    owner = ids // table_rows
    earlier = jnp.arange(rows)[None, :] < jnp.arange(rows)[:, None]
    rank = jnp.sum(((owner[:, None] == owner[None, :]) & earlier).astype(I32), 1)
    padded = jnp.pad(asked, ((0, 0), (0, cap)))

    def more(state):
        turn, held = state
        offsets = lax.dynamic_slice_in_dim(padded, turn * cap, cap, 1)
        arrived = exchange(offsets).reshape(n_shard * cap, width)
        place = jnp.where(rank // cap == turn, owner * cap + rank - turn * cap, -1)
        chosen = (place[:, None] == jnp.arange(n_shard * cap)[None, :]).astype(BF16)
        return turn + 1, held + jnp.dot(chosen, arrived, preferred_element_type=F32).astype(BF16)

    extra = lax.while_loop(
        lambda state: state[0] < rounds, more, (jnp.int32(1), jnp.zeros((rows, width), BF16))
    )[1]

    center = centroids[cent_ids.reshape(-1)]
    docs = decode(bucket_weights, lengths, residual_words, center)

    emb = encode(
        recv,
        extra,
        ids,
        pos_table,
        (emb_gain, emb_bias, b_qkv, ln1_gain, ln1_bias, b_up, ln2_gain, ln2_bias),
        (w_qkv, w_out, w_up, w_down, w_proj),
        cap,
        table_rows,
    )

    half = n_shard // 2
    odd = shard % 2
    place = shard // 2
    turns = [[2 * j + p for j in range(half)] for p in range(2)]
    swap = [(i, i ^ 1) for i in range(n_shard)]
    by_group = lax.all_to_all(
        jnp.broadcast_to(emb[None], (n_group,) + emb.shape),
        "group",
        split_axis=0,
        concat_axis=0,
        tiled=True,
    )
    other_group = lax.ppermute(by_group, "shard", swap)
    by_row = lax.all_to_all(
        jnp.broadcast_to(by_group[None], (half,) + by_group.shape),
        "shard",
        split_axis=0,
        concat_axis=0,
        tiled=True,
        axis_index_groups=turns,
    ).reshape((half * n_group,) + emb.shape)
    other_row = lax.ppermute(by_row, "shard", swap)
    groups = jnp.arange(n_group, dtype=I32)
    at = groups * n_shard + 2 * place
    away = (place + 1 + jnp.arange(half - 1, dtype=I32)) % half
    source = (away[:, None] * n_group + groups[None, :]).reshape(-1)
    target = (groups[None, :] * n_shard + 2 * away[:, None]).reshape(-1)
    run = functools.partial(maxsim, docs=docs, devices=devices, plen=plen, qlen=qlen)
    scores = run(by_group, groups, at + odd, previous=None)
    scores = run(other_group, groups, at + 1 - odd, previous=scores)
    scores = run(by_row, source, target + odd, previous=scores)
    scores = run(other_row, source, target + 1 - odd, previous=scores)
    returned = lax.all_to_all(scores, BOTH, split_axis=0, concat_axis=0, tiled=True)
    result = select(
        returned.reshape(devices * q_dev, -1),
        cand_store.reshape(-1, 1),
        cand_local.reshape(-1, many),
        q_dev,
    )
    return result.reshape(cand_local.shape)


def solution(mesh):
    rows = P(BOTH)
    placed = (rows, P("shard")) + (P(),) * 16 + (rows,) * 5
    return jax.shard_map(
        on_device, mesh=mesh, in_specs=placed, out_specs=rows, check_vma=False
    )
```

```python
import functools

import jax
import jax.numpy as jnp
from jax import lax
from jax.experimental import pallas as pl
from jax.experimental.pallas import tpu as pltpu
from jax.sharding import PartitionSpec as P

HEADS = 12
LN_EPS = 1e-12
UNIT_EPS = 1e-06
F32 = jnp.float32
BF16 = jnp.bfloat16
I32 = jnp.int32
VM = pl.BlockSpec(memory_space=pltpu.VMEM)
ANY = pl.BlockSpec(memory_space=pltpu.HBM)
SM = pl.BlockSpec(memory_space=pltpu.SMEM)
BOTH = ("group", "shard")


def grant(mebibytes):
    return pltpu.CompilerParams(vmem_limit_bytes=mebibytes * 1024 * 1024)


def pin(array):
    return pltpu.with_memory_space_constraint(array, pltpu.HBM)


def dot(lhs, rhs):
    return jnp.dot(lhs, rhs, preferred_element_type=F32)


def dot_t(lhs, rhs):
    return lax.dot_general(lhs, rhs, (((1,), (1,)), ((), ())), preferred_element_type=F32)


def iota(shape, dim):
    return lax.broadcasted_iota(I32, shape, dim)


def three(values):
    high = values.astype(BF16)
    rest = values - high.astype(F32)
    mid = rest.astype(BF16)
    return high, mid, (rest - mid.astype(F32)).astype(BF16)


def layer_norm(values, gain, bias):
    center = values - jnp.mean(values, -1, keepdims=True)
    spread = jnp.mean(center * center, -1, keepdims=True)
    return center * lax.rsqrt(spread + LN_EPS) * gain + bias


def route_kernel(
    me_ref, ids_ref, table_hbm, rows_ref, list_ref, most_ref, table, ids, fresh, chosen_ref, sems, *, cap
):
    n_dest, _, tokens = ids_ref.shape
    table_rows, width = table.shape
    parts = sems.shape[0]
    part = table_rows // parts
    copies = []
    for k in range(parts):
        piece = pl.ds(k * part, part)
        copies.append(pltpu.make_async_copy(table_hbm.at[piece], table.at[piece], sems.at[k]))
        copies[-1].start()
    for dest in range(n_dest):
        ids[dest : dest + 1, :] = ids_ref[dest]
    every = ids[...]
    columns = every.astype(F32).T
    earlier = iota((tokens, tokens), 0) < iota((tokens, tokens), 1)
    before = earlier.astype(F32).astype(BF16)
    for dest in range(n_dest):
        again = (columns[:, dest : dest + 1] == every[dest : dest + 1].astype(F32)) & earlier
        fresh[dest : dest + 1, :] = 1.0 - jnp.max(again.astype(F32), 0, keepdims=True)
    new = fresh[...]
    most = jnp.float32(0)
    for owner in range(n_dest):
        held = (every >= owner * table_rows) & (every < (owner + 1) * table_rows)
        most = jnp.maximum(most, jnp.max(jnp.sum(jnp.where(held, new, 0.0), -1, keepdims=True)))
    most_ref[0] = most.astype(I32)
    offset = every - me_ref[0] * table_rows
    inside = (offset >= 0) & (offset < table_rows) & (new > 0.5)
    rank = dot(inside.astype(F32).astype(BF16), before).astype(I32)
    rank = jnp.where(inside, rank, -1)
    kept = jnp.where(inside, offset, 0)
    wide = kept.astype(F32)
    high = jnp.right_shift(kept, 7).astype(F32).astype(BF16)
    low = (kept & 127).astype(F32).astype(BF16)
    places = iota((cap, tokens), 0)
    all_places = iota((tokens, tokens), 0)
    for dest in range(n_dest):
        matches = places == rank[dest : dest + 1]
        column = jnp.sum(jnp.where(matches, wide[dest : dest + 1], 0.0), -1, keepdims=True)
        hit = iota((cap, table_rows), 1) == column.astype(I32)
        chosen_ref[dest * cap : (dest + 1) * cap, :] = hit.astype(F32).astype(BF16)
        full = (all_places == rank[dest : dest + 1]).astype(F32).astype(BF16)
        pair = jnp.concatenate([high[dest : dest + 1], low[dest : dest + 1]], 0)
        moved = dot_t(pair, full).astype(I32)
        list_ref[dest : dest + 1, :] = moved[0:1] * 128 + moved[1:2]
    for copy in copies:
        copy.wait()
    for c in range(0, width, 256):
        rows_ref[:, c : c + 256] = dot(chosen_ref[...], table[:, c : c + 256]).astype(BF16)


def route(me, all_ids, word_table, cap):
    n_dest, _, tokens = all_ids.shape
    table_rows, width = word_table.shape
    return pl.pallas_call(
        functools.partial(route_kernel, cap=cap),
        out_shape=(
            jax.ShapeDtypeStruct((n_dest * cap, width), BF16),
            jax.ShapeDtypeStruct((n_dest, tokens), I32),
            jax.ShapeDtypeStruct((1,), I32),
        ),
        in_specs=[SM, VM, ANY],
        out_specs=(VM, VM, SM),
        scratch_shapes=[
            pltpu.VMEM(word_table.shape, BF16),
            pltpu.VMEM((n_dest, tokens), I32),
            pltpu.VMEM((n_dest, tokens), F32),
            pltpu.VMEM((n_dest * cap, table_rows), BF16),
            pltpu.SemaphoreType.DMA((4 if table_rows % 64 == 0 else 1,)),
        ],
        compiler_params=grant(24),
    )(me, all_ids, word_table)


def decode_kernel(levels_ref, lengths_ref, words_ref, center_ref, docs_ref):
    many, n_words, plen = words_ref.shape
    dim = docs_ref.shape[1]
    each = dim // n_words
    spread = (iota((n_words, dim), 1) // each == iota((n_words, dim), 0)).astype(F32).astype(BF16)
    shifts = 2 * (iota((plen, dim), 1) % each)
    first = pl.program_id(0) * many
    for p in range(many):
        words = words_ref[p].astype(F32).T.astype(BF16)
        codes = jnp.right_shift(dot(words, spread).astype(I32), shifts) & 3
        residual = jnp.full(codes.shape, levels_ref[0], F32)
        for level in range(1, levels_ref.shape[0]):
            residual = jnp.where(codes == level, levels_ref[level], residual)
        summed = center_ref[p * plen : (p + 1) * plen, :].astype(F32) + residual
        unit = summed * lax.rsqrt(jnp.sum(summed * summed, -1, keepdims=True) + UNIT_EPS)
        unit = jnp.where(iota(unit.shape, 0) < lengths_ref[first + p], unit, unit[0:1])
        docs_ref[p * plen : (p + 1) * plen, :] = unit.astype(BF16)


def decode(levels, lengths, words, center):
    passages, n_words, plen = words.shape
    dim = center.shape[1]
    many = 8
    return pl.pallas_call(
        decode_kernel,
        grid=(passages // many,),
        out_shape=jax.ShapeDtypeStruct((passages * plen, dim), BF16),
        in_specs=[
            SM,
            SM,
            pl.BlockSpec((many, n_words, plen), lambda i: (i, 0, 0)),
            pl.BlockSpec((many * plen, dim), lambda i: (i, 0)),
        ],
        out_specs=pl.BlockSpec((many * plen, dim), lambda i: (i, 0)),
        compiler_params=grant(8),
    )(levels, lengths, pin(words), center)


def encode_kernel(
    recv_ref,
    extra_ref,
    row_ref,
    column_ref,
    pos_ref,
    emb_gain,
    emb_bias,
    b_qkv,
    ln1_gain,
    ln1_bias,
    b_up,
    ln2_gain,
    ln2_bias,
    w_qkv_hbm,
    w_out_hbm,
    w_up_hbm,
    w_down_hbm,
    w_proj_hbm,
    out_ref,
    w_qkv,
    w_out,
    w_up,
    w_down,
    w_proj,
    mixed_ref,
    context_ref,
    sems,
    *,
    cap,
    table_rows,
):
    copies = []
    for k, (source, target) in enumerate(
        (
            (w_qkv_hbm, w_qkv),
            (w_out_hbm, w_out),
            (w_up_hbm, w_up),
            (w_down_hbm, w_down),
            (w_proj_hbm, w_proj),
        )
    ):
        copies.append(pltpu.make_async_copy(source, target, sems.at[k]))
        copies[-1].start()
    rows, width = extra_ref.shape
    qlen = pos_ref.shape[0]
    owner_row = row_ref[...] // table_rows
    owner_column = column_ref[...] // table_rows
    down, across = iota((rows, rows), 0), iota((rows, rows), 1)
    equal = column_ref[...] == row_ref[...]
    again = jnp.max((equal & (down < across)).astype(F32), 0, keepdims=True)
    first = jnp.min(jnp.where(equal, across.astype(F32), float(rows)), -1, keepdims=True)
    same = (owner_column == owner_row) & (across.astype(F32) < first) & (again < 0.5)
    rank = jnp.sum(same.astype(F32), -1, keepdims=True).astype(I32)
    place = jnp.where(rank < cap, owner_column * cap + rank, -1)
    slots = recv_ref.shape[0]
    chosen = (iota((rows, slots), 1) == place).astype(F32).astype(BF16)
    own = dot(chosen, recv_ref[...]) + extra_ref[...].astype(F32)
    pos = pos_ref[...].astype(F32)
    embedded = own + jnp.concatenate([pos] * (rows // qlen), 0)
    hidden = layer_norm(embedded, emb_gain[...], emb_bias[...])
    copies[0].wait()
    mixed_ref[...] = (dot(hidden.astype(BF16), w_qkv[...]) + b_qkv[...]).astype(BF16)
    head = width // HEADS
    per = 128 // head
    scale = head ** (-0.5)
    outside = iota((rows, rows), 0) // qlen != iota((rows, rows), 1) // qlen
    bias = jnp.where(outside, -jnp.inf, 0.0)
    lane = iota((rows, 128), 1) // head
    for i in range(width // 128):
        query = mixed_ref[:, i * 128 : (i + 1) * 128]
        keys = mixed_ref[:, width + i * 128 : width + (i + 1) * 128]
        values = mixed_ref[:, 2 * width + i * 128 : 2 * width + (i + 1) * 128]
        context = jnp.zeros((rows, 128), F32)
        for h in range(per):
            mine = lane == h
            logits = dot_t(jnp.where(mine, query, jnp.zeros_like(query)), keys) * scale + bias
            powers = jnp.exp(logits - jnp.max(logits, -1, keepdims=True))
            probs = (powers / jnp.sum(powers, -1, keepdims=True)).astype(BF16)
            context = context + dot(probs, jnp.where(mine, values, jnp.zeros_like(values)))
        context_ref[:, i * 128 : (i + 1) * 128] = context.astype(BF16)
    copies[1].wait()
    first = layer_norm(hidden + dot(context_ref[...], w_out[...]), ln1_gain[...], ln1_bias[...])
    narrow = first.astype(BF16)
    hidden_units = w_up.shape[1]
    step = width
    copies[2].wait()
    copies[3].wait()
    total = jnp.zeros((rows, width), F32)
    for c in range(hidden_units // step):
        inner = dot(narrow, w_up[:, c * step : (c + 1) * step]) + b_up[c * step : (c + 1) * step]
        inner = 0.5 * inner * (1.0 + lax.erf(inner * (0.5**0.5)))
        total = total + dot(inner.astype(BF16), w_down[c * step : (c + 1) * step, :])
    second = layer_norm(first + total, ln2_gain[...], ln2_bias[...])
    copies[4].wait()
    projected = dot(second.astype(BF16), w_proj[...])
    unit = projected * lax.rsqrt(jnp.sum(projected * projected, -1, keepdims=True) + UNIT_EPS)
    unit = unit.T.astype(BF16)
    for k in range(out_ref.shape[0]):
        out_ref[k] = unit


def encode(recv, extra, ids, pos, vectors, weights, cap, table_rows, copies):
    rows = extra.shape[0]
    dim = weights[-1].shape[1]
    width = extra.shape[1]
    return pl.pallas_call(
        functools.partial(encode_kernel, cap=cap, table_rows=table_rows),
        out_shape=jax.ShapeDtypeStruct((copies, dim, rows), BF16),
        in_specs=[VM] * (5 + len(vectors)) + [ANY] * len(weights),
        out_specs=VM,
        scratch_shapes=[pltpu.VMEM(w.shape, BF16) for w in weights]
        + [
            pltpu.VMEM((rows, 3 * width), BF16),
            pltpu.VMEM((rows, width), BF16),
            pltpu.SemaphoreType.DMA((len(weights),)),
        ],
        compiler_params=grant(32),
    )(
        recv,
        extra,
        ids,
        ids.reshape(rows, 1),
        pin(pos),
        *[pin(v) for v in vectors],
        *[pin(w) for w in weights],
    )


def maxsim_kernel(me_ref, docs_ref, *rest, shifts, partners, plen, qlen):
    query_refs = rest[: len(shifts)]
    out_ref, part_ref, other_ref = rest[-3:]
    n_group = out_ref.shape[0]
    many, lanes = out_ref.shape[-2:]
    half, _, rows = query_refs[0].shape
    passages = docs_ref.shape[0] // plen
    tiles = rows // 128
    segment = (iota((rows, 128), 0) // qlen == iota((rows, 128), 1)).astype(F32).astype(BF16)

    def peaks(j, part_ref):
        for b, query_ref in enumerate(query_refs):
            query = query_ref[j]
            for p in range(passages):
                sims = dot(docs_ref[p * plen : (p + 1) * plen, :], query)
                peak = jnp.max(sims.reshape(plen // 8, 8, rows), 0)
                for c in range(tiles):
                    part_ref[b * tiles + c, p * 8 : (p + 1) * 8, :] = peak[
                        :, c * 128 : (c + 1) * 128
                    ]

    def sums(j, part_ref):
        for b, (shift, partner) in enumerate(zip(shifts, partners)):
            bests = []
            for c in range(tiles):
                best = part_ref[b * tiles + c, pl.ds(0, passages, stride=8), :]
                for s in range(1, 8):
                    best = jnp.maximum(
                        best, part_ref[b * tiles + c, pl.ds(s, passages, stride=8), :]
                    )
                bests.append(best)
            best = jnp.concatenate(bests, 1)
            total = dot(jnp.concatenate(three(best), 0), segment)
            total = total[:passages] + (
                total[passages : 2 * passages] + total[2 * passages :]
            )
            group = lax.rem(me_ref[1] + n_group - shift, n_group)
            side = lax.rem(me_ref[0] + partner, 2)
            turned = total.T[:many]
            if lanes > passages:
                turned = jnp.concatenate(
                    [turned, jnp.zeros((many, lanes - passages), F32)], 1
                )
            out_ref[group, j, side] = turned

    other_ref[...] = jnp.zeros_like(other_ref)

    def step(i, carry):
        peaks(2 * i, part_ref)
        sums(jnp.maximum(2 * i - 1, 0), other_ref)
        peaks(2 * i + 1, other_ref)
        sums(2 * i, part_ref)
        return carry

    lax.fori_loop(0, half // 2, step, 0)
    sums(2 * (half // 2) - 1, other_ref)
    if half % 2:
        peaks(half - 1, part_ref)
        sums(half - 1, part_ref)


def maxsim(me, docs, queries, shifts, partners, previous, n_group, plen, qlen):
    half, dim, rows = queries[0].shape
    passages = docs.shape[0] // plen
    lanes = -(-passages // 128) * 128
    shape = (n_group, half, 2, rows // qlen, lanes)
    extra = [] if previous is None else [previous]
    many = len(queries)
    return pl.pallas_call(
        functools.partial(
            maxsim_kernel, shifts=shifts, partners=partners, plen=plen, qlen=qlen
        ),
        out_shape=jax.ShapeDtypeStruct(shape, F32),
        in_specs=[SM] + [VM] * (1 + many + len(extra)),
        out_specs=VM,
        scratch_shapes=[pltpu.VMEM((many * rows // 128, passages * 8, 128), F32)] * 2,
        input_output_aliases={2 + many: 0} if extra else {},
        compiler_params=grant(8),
        cost_estimate=pl.CostEstimate(
            flops=2 * many * half * rows * docs.size, transcendentals=0, bytes_accessed=docs.size
        ),
    )(me, docs, *queries, *extra)


def select_kernel(table_ref, store_ref, local_ref, out_ref, store, local, *, passages):
    picks, q_dev, each = local_ref.shape
    rows = table_ref.shape[0]
    pairs = q_dev * each
    for q in range(q_dev):
        store[0:1, q * each : (q + 1) * each] = store_ref[q : q + 1, :] * q_dev + q
        local[:, q * each : (q + 1) * each] = local_ref[:, q, :]
    chosen = (iota((rows, pairs), 0) == store[...]).astype(F32).astype(BF16)
    high, mid, low = three(table_ref[...].T[:passages])
    own = dot(high, chosen) + (dot(mid, chosen) + dot(low, chosen))
    wanted = local[...]
    result = jnp.zeros(wanted.shape, F32)
    for p in range(passages):
        result = jnp.where(wanted == p, own[p : p + 1], result)
    for q in range(q_dev):
        out_ref[:, q, :] = result[:, q * each : (q + 1) * each]


def select(table, store, local, passages):
    picks, q_dev, each = local.shape
    return pl.pallas_call(
        functools.partial(select_kernel, passages=passages),
        out_shape=jax.ShapeDtypeStruct(local.shape, F32),
        in_specs=[VM] * 3,
        out_specs=VM,
        scratch_shapes=[pltpu.VMEM((1, q_dev * each), I32), pltpu.VMEM((picks, q_dev * each), I32)],
        compiler_params=grant(4),
    )(table, store, local)


def on_device(
    query_ids,
    word_table,
    pos_table,
    emb_gain,
    emb_bias,
    w_qkv,
    b_qkv,
    w_out,
    ln1_gain,
    ln1_bias,
    w_up,
    b_up,
    w_down,
    ln2_gain,
    ln2_bias,
    w_proj,
    centroids,
    bucket_weights,
    cand_store,
    cand_local,
    cent_ids,
    residual_words,
    lengths,
):
    n_group = lax.axis_size("group")
    n_shard = lax.axis_size("shard")
    devices = n_group * n_shard
    q_dev, qlen = query_ids.shape
    table_rows, width = word_table.shape
    rows = q_dev * qlen
    passages, plen = cent_ids.shape
    cap = -(-3 * rows // (2 * n_shard) // 16) * 16
    me = jnp.stack([lax.axis_index("shard"), lax.axis_index("group")]).astype(I32)

    ids = query_ids.reshape(1, rows)
    all_ids = lax.all_gather(ids, "shard", axis=0)
    looked, asked, most = route(me, all_ids, word_table, cap)

    def exchange(sent):
        sent = sent.reshape(n_shard, cap, width)
        arrived = lax.all_to_all(sent, "shard", split_axis=0, concat_axis=0, tiled=True)
        return arrived.reshape(n_shard * cap, width)

    recv = exchange(looked)

    rounds = (most[0] + cap - 1) // cap

    def more(state):
        turn, held = state
        padded = jnp.pad(asked, ((0, 0), (0, cap)))
        offsets = lax.dynamic_slice_in_dim(padded, turn * cap, cap, 1)
        arrived = exchange(word_table[offsets.reshape(-1)])
        owner = query_ids.reshape(rows) // table_rows
        equal = ids.reshape(rows, 1) == ids
        across = jnp.arange(rows, dtype=I32)
        new = jnp.logical_not(jnp.any(equal & (across[:, None] < across[None, :]), 0))
        first = jnp.min(jnp.where(equal, across[None, :], rows), 1)
        same = (owner[:, None] == owner[None, :]) & (across[None, :] < first[:, None]) & new[None, :]
        rank = jnp.sum(same.astype(I32), 1)
        place = jnp.where(rank // cap == turn, owner * cap + rank - turn * cap, -1)
        chosen = (place[:, None] == jnp.arange(n_shard * cap)[None, :]).astype(BF16)
        return turn + 1, held + jnp.dot(chosen, arrived, preferred_element_type=F32).astype(BF16)

    extra = lax.while_loop(
        lambda state: state[0] < rounds, more, (jnp.int32(1), jnp.zeros((rows, width), BF16))
    )[1]

    center = centroids[cent_ids.reshape(-1)]
    recv, center = lax.optimization_barrier((recv, center))
    emb = encode(
        recv,
        extra,
        ids,
        pos_table,
        (emb_gain, emb_bias, b_qkv, ln1_gain, ln1_bias, b_up, ln2_gain, ln2_bias),
        (w_qkv, w_out, w_up, w_down, w_proj),
        cap,
        table_rows,
        n_shard // 2,
    )
    emb, center = lax.optimization_barrier((emb, center))

    half = n_shard // 2
    turns = [[2 * j + p for j in range(half)] for p in range(2)]
    swap = [(i, i ^ 1) for i in range(n_shard)]

    def partner(block):
        return lax.ppermute(block, "shard", swap)

    def back(block, shift):
        pairs = [(i, (i + shift) % n_group) for i in range(n_group)]
        return lax.ppermute(block, "group", pairs)

    row = lax.all_to_all(
        emb, "shard", split_axis=0, concat_axis=0, tiled=True, axis_index_groups=turns
    )
    docs = decode(bucket_weights, lengths, residual_words, center)
    row, docs = lax.optimization_barrier((row, docs))
    run = functools.partial(maxsim, me, docs, n_group=n_group, plen=plen, qlen=qlen)
    waves = [(k, n_group - k) for k in range(1, (n_group + 1) // 2)]
    waves += [(n_group // 2,)] if n_group % 2 == 0 else []
    blocks = {k: back(row, k) for wave in waves for k in wave}
    scores = run((row, partner(row)), (0, 0), (0, 1), None)
    for wave in waves:
        here = tuple(blocks[k] for k in wave)
        here, scores = lax.optimization_barrier((here, scores))
        there = tuple(partner(block) for block in here)
        scores = run(here, wave, (0,) * len(wave), scores)
        scores = run(there, wave, (1,) * len(wave), scores)
    scores = scores.reshape((devices,) + scores.shape[3:])
    returned = lax.all_to_all(scores, BOTH, split_axis=0, concat_axis=0, tiled=True)
    result = select(
        returned.reshape(devices * q_dev, -1),
        cand_store,
        jnp.transpose(cand_local, (2, 0, 1)),
        passages,
    )
    return jnp.transpose(result, (1, 2, 0))


def solution(mesh):
    rows = P(BOTH)
    placed = (rows, P("shard")) + (P(),) * 16 + (rows,) * 5
    return jax.shard_map(
        on_device, mesh=mesh, in_specs=placed, out_specs=rows, check_vma=False
    )
```

```python
import functools

import jax
import jax.numpy as jnp
from jax import lax
from jax.experimental import pallas as pl
from jax.experimental.pallas import tpu as pltpu
from jax.sharding import PartitionSpec as P

HEADS = 12
LN_EPS = 1e-12
UNIT_EPS = 1e-06
F32 = jnp.float32
BF16 = jnp.bfloat16
I32 = jnp.int32
VM = pl.BlockSpec(memory_space=pltpu.VMEM)
ANY = pl.BlockSpec(memory_space=pltpu.HBM)
SM = pl.BlockSpec(memory_space=pltpu.SMEM)
BOTH = ("group", "shard")


def grant(mebibytes):
    return pltpu.CompilerParams(vmem_limit_bytes=mebibytes * 1024 * 1024)


def pin(array):
    return pltpu.with_memory_space_constraint(array, pltpu.HBM)


def dot(lhs, rhs):
    return jnp.dot(lhs, rhs, preferred_element_type=F32)


def dot_t(lhs, rhs):
    return lax.dot_general(lhs, rhs, (((1,), (1,)), ((), ())), preferred_element_type=F32)


def iota(shape, dim):
    return lax.broadcasted_iota(I32, shape, dim)


def three(values):
    high = values.astype(BF16)
    rest = values - high.astype(F32)
    mid = rest.astype(BF16)
    return high, mid, (rest - mid.astype(F32)).astype(BF16)


def layer_norm(values, gain, bias):
    center = values - jnp.mean(values, -1, keepdims=True)
    spread = jnp.mean(center * center, -1, keepdims=True)
    return center * lax.rsqrt(spread + LN_EPS) * gain + bias


def route_kernel(
    me_ref, ids_ref, table_hbm, rows_ref, list_ref, most_ref, table, ids, fresh, chosen_ref, sems, *, cap
):
    n_dest, q_dev, qlen = ids_ref.shape
    tokens = q_dev * qlen
    table_rows, width = table.shape
    parts = sems.shape[0]
    part = table_rows // parts
    copies = []
    for k in range(parts):
        piece = pl.ds(k * part, part)
        copies.append(pltpu.make_async_copy(table_hbm.at[piece], table.at[piece], sems.at[k]))
        copies[-1].start()
    for q in range(q_dev):
        ids[:, q * qlen : (q + 1) * qlen] = ids_ref[:, q, :]
    every = ids[...]
    columns = every.astype(F32).T
    earlier = iota((tokens, tokens), 0) < iota((tokens, tokens), 1)
    before = earlier.astype(F32).astype(BF16)
    for dest in range(n_dest):
        again = (columns[:, dest : dest + 1] == every[dest : dest + 1].astype(F32)) & earlier
        fresh[dest : dest + 1, :] = 1.0 - jnp.max(again.astype(F32), 0, keepdims=True)
    new = fresh[...]
    most = jnp.float32(0)
    for owner in range(n_dest):
        held = (every >= owner * table_rows) & (every < (owner + 1) * table_rows)
        most = jnp.maximum(most, jnp.max(jnp.sum(jnp.where(held, new, 0.0), -1, keepdims=True)))
    most_ref[0] = most.astype(I32)
    offset = every - me_ref[0] * table_rows
    inside = (offset >= 0) & (offset < table_rows) & (new > 0.5)
    rank = dot(inside.astype(F32).astype(BF16), before).astype(I32)
    rank = jnp.where(inside, rank, -1)
    kept = jnp.where(inside, offset, 0)
    wide = kept.astype(F32)
    high = jnp.right_shift(kept, 7).astype(F32).astype(BF16)
    low = (kept & 127).astype(F32).astype(BF16)
    places = iota((cap, tokens), 0)
    all_places = iota((tokens, tokens), 0)
    for dest in range(n_dest):
        matches = places == rank[dest : dest + 1]
        column = jnp.sum(jnp.where(matches, wide[dest : dest + 1], 0.0), -1, keepdims=True)
        hit = iota((cap, table_rows), 1) == column.astype(I32)
        chosen_ref[dest * cap : (dest + 1) * cap, :] = hit.astype(F32).astype(BF16)
        full = (all_places == rank[dest : dest + 1]).astype(F32).astype(BF16)
        pair = jnp.concatenate([high[dest : dest + 1], low[dest : dest + 1]], 0)
        moved = dot_t(pair, full).astype(I32)
        list_ref[dest : dest + 1, :] = moved[0:1] * 128 + moved[1:2]
    for copy in copies:
        copy.wait()
    for c in range(0, width, 256):
        rows_ref[:, c : c + 256] = dot(chosen_ref[...], table[:, c : c + 256]).astype(BF16)


def route(me, all_ids, word_table, cap):
    n_dest, tokens = all_ids.shape[0], all_ids.shape[1] * all_ids.shape[2]
    table_rows, width = word_table.shape
    return pl.pallas_call(
        functools.partial(route_kernel, cap=cap),
        out_shape=(
            jax.ShapeDtypeStruct((n_dest * cap, width), BF16),
            jax.ShapeDtypeStruct((n_dest, tokens), I32),
            jax.ShapeDtypeStruct((1,), I32),
        ),
        in_specs=[SM, VM, ANY],
        out_specs=(VM, VM, SM),
        scratch_shapes=[
            pltpu.VMEM(word_table.shape, BF16),
            pltpu.VMEM((n_dest, tokens), I32),
            pltpu.VMEM((n_dest, tokens), F32),
            pltpu.VMEM((n_dest * cap, table_rows), BF16),
            pltpu.SemaphoreType.DMA((4 if table_rows % 64 == 0 else 1,)),
        ],
        compiler_params=grant(24),
    )(me, all_ids, word_table)


def decode_kernel(levels_ref, lengths_ref, words_ref, center_ref, docs_ref):
    many, n_words, plen = words_ref.shape
    dim = docs_ref.shape[1]
    each = dim // n_words
    spread = (iota((n_words, dim), 1) // each == iota((n_words, dim), 0)).astype(F32).astype(BF16)
    shifts = 2 * (iota((plen, dim), 1) % each)
    first = pl.program_id(0) * many
    for p in range(many):
        words = words_ref[p].astype(F32).T.astype(BF16)
        codes = jnp.right_shift(dot(words, spread).astype(I32), shifts) & 3
        residual = jnp.full(codes.shape, levels_ref[0], F32)
        for level in range(1, levels_ref.shape[0]):
            residual = jnp.where(codes == level, levels_ref[level], residual)
        summed = center_ref[p * plen : (p + 1) * plen, :].astype(F32) + residual
        unit = summed * lax.rsqrt(jnp.sum(summed * summed, -1, keepdims=True) + UNIT_EPS)
        unit = jnp.where(iota(unit.shape, 0) < lengths_ref[first + p], unit, unit[0:1])
        docs_ref[p * plen : (p + 1) * plen, :] = unit.astype(BF16)


def decode(levels, lengths, words, center):
    passages, n_words, plen = words.shape
    dim = center.shape[1]
    many = 8
    return pl.pallas_call(
        decode_kernel,
        grid=(passages // many,),
        out_shape=jax.ShapeDtypeStruct((passages * plen, dim), BF16),
        in_specs=[
            SM,
            SM,
            pl.BlockSpec((many, n_words, plen), lambda i: (i, 0, 0)),
            pl.BlockSpec((many * plen, dim), lambda i: (i, 0)),
        ],
        out_specs=pl.BlockSpec((many * plen, dim), lambda i: (i, 0)),
        compiler_params=grant(8),
    )(levels, lengths, pin(words), center)


def encode_kernel(
    recv_ref,
    extra_ref,
    row_ref,
    column_ref,
    pos_ref,
    emb_gain,
    emb_bias,
    b_qkv,
    ln1_gain,
    ln1_bias,
    b_up,
    ln2_gain,
    ln2_bias,
    w_qkv_hbm,
    w_out_hbm,
    w_up_hbm,
    w_down_hbm,
    w_proj_hbm,
    out_ref,
    w_qkv,
    w_out,
    w_up,
    w_down,
    w_proj,
    mixed_ref,
    context_ref,
    sems,
    *,
    cap,
    table_rows,
):
    copies = []
    for k, (source, target) in enumerate(
        (
            (w_qkv_hbm, w_qkv),
            (w_out_hbm, w_out),
            (w_up_hbm, w_up),
            (w_down_hbm, w_down),
            (w_proj_hbm, w_proj),
        )
    ):
        copies.append(pltpu.make_async_copy(source, target, sems.at[k]))
    copies[0].start()
    rows, width = extra_ref.shape
    qlen = pos_ref.shape[0]
    owner_row = row_ref[...] // table_rows
    owner_column = column_ref[...] // table_rows
    down, across = iota((rows, rows), 0), iota((rows, rows), 1)
    equal = column_ref[...] == row_ref[...]
    again = jnp.max((equal & (down < across)).astype(F32), 0, keepdims=True)
    first = jnp.min(jnp.where(equal, across.astype(F32), float(rows)), -1, keepdims=True)
    same = (owner_column == owner_row) & (across.astype(F32) < first) & (again < 0.5)
    rank = jnp.sum(same.astype(F32), -1, keepdims=True).astype(I32)
    place = jnp.where(rank < cap, owner_column * cap + rank, -1)
    slots = recv_ref.shape[0]
    chosen = (iota((rows, slots), 1) == place).astype(F32).astype(BF16)
    own = dot(chosen, recv_ref[...]) + extra_ref[...].astype(F32)
    pos = pos_ref[...].astype(F32)
    embedded = own + jnp.concatenate([pos] * (rows // qlen), 0)
    hidden = layer_norm(embedded, emb_gain[...], emb_bias[...])
    copies[0].wait()
    for copy in copies[1:]:
        copy.start()
    mixed_ref[...] = (dot(hidden.astype(BF16), w_qkv[...]) + b_qkv[...]).astype(BF16)
    head = width // HEADS
    per = 128 // head
    scale = head ** (-0.5)
    outside = iota((rows, rows), 0) // qlen != iota((rows, rows), 1) // qlen
    bias = jnp.where(outside, -jnp.inf, 0.0)
    lane = iota((rows, 128), 1) // head
    for i in range(width // 128):
        query = mixed_ref[:, i * 128 : (i + 1) * 128]
        keys = mixed_ref[:, width + i * 128 : width + (i + 1) * 128]
        values = mixed_ref[:, 2 * width + i * 128 : 2 * width + (i + 1) * 128]
        context = jnp.zeros((rows, 128), F32)
        for h in range(per):
            mine = lane == h
            logits = dot_t(jnp.where(mine, query, jnp.zeros_like(query)), keys) * scale + bias
            powers = jnp.exp(logits - jnp.max(logits, -1, keepdims=True))
            probs = (powers / jnp.sum(powers, -1, keepdims=True)).astype(BF16)
            context = context + dot(probs, jnp.where(mine, values, jnp.zeros_like(values)))
        context_ref[:, i * 128 : (i + 1) * 128] = context.astype(BF16)
    copies[1].wait()
    first = layer_norm(hidden + dot(context_ref[...], w_out[...]), ln1_gain[...], ln1_bias[...])
    narrow = first.astype(BF16)
    hidden_units = w_up.shape[1]
    step = width
    copies[2].wait()
    copies[3].wait()
    total = jnp.zeros((rows, width), F32)
    for c in range(hidden_units // step):
        inner = dot(narrow, w_up[:, c * step : (c + 1) * step]) + b_up[c * step : (c + 1) * step]
        inner = 0.5 * inner * (1.0 + lax.erf(inner * (0.5**0.5)))
        total = total + dot(inner.astype(BF16), w_down[c * step : (c + 1) * step, :])
    second = layer_norm(first + total, ln2_gain[...], ln2_bias[...])
    copies[4].wait()
    projected = dot(second.astype(BF16), w_proj[...])
    unit = projected * lax.rsqrt(jnp.sum(projected * projected, -1, keepdims=True) + UNIT_EPS)
    out_ref[...] = unit.T.astype(BF16)


def encode(recv, extra, ids, pos, vectors, weights, cap, table_rows):
    rows = extra.shape[0]
    dim = weights[-1].shape[1]
    width = extra.shape[1]
    return pl.pallas_call(
        functools.partial(encode_kernel, cap=cap, table_rows=table_rows),
        out_shape=jax.ShapeDtypeStruct((dim, rows), BF16),
        in_specs=[VM] * (5 + len(vectors)) + [ANY] * len(weights),
        out_specs=VM,
        scratch_shapes=[pltpu.VMEM(w.shape, BF16) for w in weights]
        + [
            pltpu.VMEM((rows, 3 * width), BF16),
            pltpu.VMEM((rows, width), BF16),
            pltpu.SemaphoreType.DMA((len(weights),)),
        ],
        compiler_params=grant(32),
    )(
        recv,
        extra,
        ids,
        ids.reshape(rows, 1),
        pin(pos),
        *[pin(v) for v in vectors],
        *[pin(w) for w in weights],
    )


def met(place, step, half, backwards=False):
    if half & (half - 1) == 0:
        return place ^ step
    return (place + (half - step if backwards else step)) % half


def maxsim_kernel(me_ref, docs_ref, *rest, moves, partners, plen, qlen):
    query_refs = rest[: len(moves)]
    out_ref, part_ref, other_ref = rest[-3:]
    n_group, places = out_ref.shape[:2]
    many, lanes = out_ref.shape[-2:]
    half, _, rows = query_refs[0].shape
    passages = docs_ref.shape[0] // plen
    tiles = rows // 128
    segment = (iota((rows, 128), 0) // qlen == iota((rows, 128), 1)).astype(F32).astype(BF16)

    def peaks(j, part_ref):
        for b, query_ref in enumerate(query_refs):
            query = query_ref[j]
            for p in range(passages):
                sims = dot(docs_ref[p * plen : (p + 1) * plen, :], query)
                peak = jnp.max(sims.reshape(plen // 8, 8, rows), 0)
                for c in range(tiles):
                    part_ref[b * tiles + c, p * 8 : (p + 1) * 8, :] = peak[
                        :, c * 128 : (c + 1) * 128
                    ]

    def sums(j, part_ref):
        for b, (move, partner) in enumerate(zip(moves, partners)):
            bests = []
            for c in range(tiles):
                best = part_ref[b * tiles + c, pl.ds(0, passages, stride=8), :]
                for s in range(1, 8):
                    best = jnp.maximum(
                        best, part_ref[b * tiles + c, pl.ds(s, passages, stride=8), :]
                    )
                bests.append(best)
            best = jnp.concatenate(bests, 1)
            total = dot(jnp.concatenate(three(best), 0), segment)
            total = total[:passages] + (
                total[passages : 2 * passages] + total[2 * passages :]
            )
            group = lax.rem(me_ref[1] + n_group - j, n_group)
            place = met(me_ref[0] // 2, move, places, True)
            side = lax.rem(me_ref[0] + partner, 2)
            turned = total.T[:many]
            if lanes > passages:
                turned = jnp.concatenate(
                    [turned, jnp.zeros((many, lanes - passages), F32)], 1
                )
            out_ref[group, place, side] = turned

    other_ref[...] = jnp.zeros_like(other_ref)

    def step(i, carry):
        peaks(2 * i, part_ref)
        sums(jnp.maximum(2 * i - 1, 0), other_ref)
        peaks(2 * i + 1, other_ref)
        sums(2 * i, part_ref)
        return carry

    if half > 1:
        lax.fori_loop(0, half // 2, step, 0)
        sums(2 * (half // 2) - 1, other_ref)
    if half % 2:
        peaks(half - 1, part_ref)
        sums(half - 1, part_ref)


def maxsim(me, docs, queries, moves, partners, previous, n_group, half, plen, qlen):
    held, dim, rows = queries[0].shape
    passages = docs.shape[0] // plen
    lanes = -(-passages // 128) * 128
    shape = (n_group, half, 2, rows // qlen, lanes)
    extra = [] if previous is None else [previous]
    many = len(queries)
    return pl.pallas_call(
        functools.partial(
            maxsim_kernel,
            moves=moves,
            partners=partners,
            plen=plen,
            qlen=qlen,
        ),
        out_shape=jax.ShapeDtypeStruct(shape, F32),
        in_specs=[SM] + [VM] * (1 + many + len(extra)),
        out_specs=VM,
        scratch_shapes=[pltpu.VMEM((many * rows // 128, passages * 8, 128), F32)] * 2,
        input_output_aliases={2 + many: 0} if extra else {},
        compiler_params=grant(8),
        cost_estimate=pl.CostEstimate(
            flops=2 * many * held * rows * docs.size, transcendentals=0, bytes_accessed=docs.size
        ),
    )(me, docs, *queries, *extra)


def select_kernel(table_ref, store_ref, local_ref, out_ref, store, local, *, passages):
    picks, q_dev, each = local_ref.shape
    rows = table_ref.shape[0]
    pairs = q_dev * each
    for q in range(q_dev):
        store[0:1, q * each : (q + 1) * each] = store_ref[q : q + 1, :] * q_dev + q
        local[:, q * each : (q + 1) * each] = local_ref[:, q, :]
    chosen = (iota((rows, pairs), 0) == store[...]).astype(F32).astype(BF16)
    high, mid, low = three(table_ref[...].T[:passages])
    own = dot(high, chosen) + (dot(mid, chosen) + dot(low, chosen))
    wanted = local[...]
    result = jnp.zeros(wanted.shape, F32)
    for p in range(passages):
        result = jnp.where(wanted == p, own[p : p + 1], result)
    for q in range(q_dev):
        out_ref[:, q, :] = result[:, q * each : (q + 1) * each]


def select(table, store, local, passages):
    picks, q_dev, each = local.shape
    return pl.pallas_call(
        functools.partial(select_kernel, passages=passages),
        out_shape=jax.ShapeDtypeStruct(local.shape, F32),
        in_specs=[VM] * 3,
        out_specs=VM,
        scratch_shapes=[pltpu.VMEM((1, q_dev * each), I32), pltpu.VMEM((picks, q_dev * each), I32)],
        compiler_params=grant(4),
    )(table, store, local)


def on_device(
    query_ids,
    word_table,
    pos_table,
    emb_gain,
    emb_bias,
    w_qkv,
    b_qkv,
    w_out,
    ln1_gain,
    ln1_bias,
    w_up,
    b_up,
    w_down,
    ln2_gain,
    ln2_bias,
    w_proj,
    centroids,
    bucket_weights,
    cand_store,
    cand_local,
    cent_ids,
    residual_words,
    lengths,
):
    n_group = lax.axis_size("group")
    n_shard = lax.axis_size("shard")
    devices = n_group * n_shard
    q_dev, qlen = query_ids.shape
    table_rows, width = word_table.shape
    rows = q_dev * qlen
    passages, plen = cent_ids.shape
    cap = -(-3 * rows // (2 * n_shard) // 16) * 16
    me = jnp.stack([lax.axis_index("shard"), lax.axis_index("group")]).astype(I32)

    ids = query_ids.reshape(1, rows)
    all_ids = lax.all_gather(query_ids, "shard", axis=0)
    looked, asked, most = route(me, all_ids, word_table, cap)

    def exchange(sent):
        sent = sent.reshape(n_shard, cap, width)
        arrived = lax.all_to_all(sent, "shard", split_axis=0, concat_axis=0, tiled=True)
        return arrived.reshape(n_shard * cap, width)

    recv = exchange(looked)

    rounds = (most[0] + cap - 1) // cap

    def more(state):
        turn, held = state
        padded = jnp.pad(asked, ((0, 0), (0, cap)))
        offsets = lax.dynamic_slice_in_dim(padded, turn * cap, cap, 1)
        arrived = exchange(word_table[offsets.reshape(-1)])
        owner = query_ids.reshape(rows) // table_rows
        equal = ids.reshape(rows, 1) == ids
        across = jnp.arange(rows, dtype=I32)
        new = jnp.logical_not(jnp.any(equal & (across[:, None] < across[None, :]), 0))
        first = jnp.min(jnp.where(equal, across[None, :], rows), 1)
        same = (owner[:, None] == owner[None, :]) & (across[None, :] < first[:, None]) & new[None, :]
        rank = jnp.sum(same.astype(I32), 1)
        place = jnp.where(rank // cap == turn, owner * cap + rank - turn * cap, -1)
        chosen = (place[:, None] == jnp.arange(n_shard * cap)[None, :]).astype(BF16)
        return turn + 1, held + jnp.dot(chosen, arrived, preferred_element_type=F32).astype(BF16)

    extra = lax.while_loop(
        lambda state: state[0] < rounds, more, (jnp.int32(1), jnp.zeros((rows, width), BF16))
    )[1]

    center = centroids[cent_ids.reshape(-1)]
    recv, center = lax.optimization_barrier((recv, center))
    emb = encode(
        recv,
        extra,
        ids,
        pos_table,
        (emb_gain, emb_bias, b_qkv, ln1_gain, ln1_bias, b_up, ln2_gain, ln2_bias),
        (w_qkv, w_out, w_up, w_down, w_proj),
        cap,
        table_rows,
    )
    emb, center = lax.optimization_barrier((emb, center))

    half = n_shard // 2
    swap = [(i, i ^ 1) for i in range(n_shard)]

    def partner(block):
        return lax.ppermute(block, "shard", swap)

    def around(step):
        pairs = [(i, (i + step) % n_group) for i in range(n_group)]
        return lax.ppermute(emb, "group", pairs)

    def across(block, step):
        pairs = [(i, 2 * met(i // 2, step, half) + i % 2) for i in range(n_shard)]
        return lax.ppermute(block, "shard", pairs)

    others = [around(k) for k in range(1, n_group)]
    docs = decode(bucket_weights, lengths, residual_words, center)
    others, docs = lax.optimization_barrier((others, docs))
    column = jnp.stack([emb] + list(others))
    run = functools.partial(
        maxsim, me, docs, n_group=n_group, half=half, plen=plen, qlen=qlen
    )
    steps = [tuple(range(k, min(k + 2, half))) for k in range(1, half, 2)]
    here, sent = (column,), column
    moves = (0,)
    scores = None
    for following in steps + [()]:
        coming = tuple(across(sent, k) for k in following)
        there = tuple(partner(block) for block in here)
        if len(here) == 1 and scores is None:
            scores = run(here + there, moves * 2, (0, 1), scores)
        else:
            scores = run(here, moves, (0,) * len(here), scores)
            scores = run(there, moves, (1,) * len(here), scores)
        if following:
            coming, sent, scores = lax.optimization_barrier((coming, column, scores))
        here, moves = coming, following
    scores = scores.reshape((devices,) + scores.shape[3:])
    returned = lax.all_to_all(scores, BOTH, split_axis=0, concat_axis=0, tiled=True)
    result = select(
        returned.reshape(devices * q_dev, -1),
        cand_store,
        jnp.transpose(cand_local, (2, 0, 1)),
        passages,
    )
    return jnp.transpose(result, (1, 2, 0))


def solution(mesh):
    rows = P(BOTH)
    placed = (rows, P("shard")) + (P(),) * 16 + (rows,) * 5
    return jax.shard_map(
        on_device, mesh=mesh, in_specs=placed, out_specs=rows, check_vma=False
    )
```

```python
import functools

import jax
import jax.numpy as jnp
from jax import lax
from jax.experimental import pallas as pl
from jax.experimental.pallas import tpu as pltpu
from jax.sharding import PartitionSpec as P

HEADS = 12
LN_EPS = 1e-12
UNIT_EPS = 1e-06
F32 = jnp.float32
BF16 = jnp.bfloat16
I32 = jnp.int32
VM = pl.BlockSpec(memory_space=pltpu.VMEM)
ANY = pl.BlockSpec(memory_space=pltpu.HBM)
SM = pl.BlockSpec(memory_space=pltpu.SMEM)
BOTH = ("group", "shard")
PIECES = 4


def grant(mebibytes):
    return pltpu.CompilerParams(vmem_limit_bytes=mebibytes * 1024 * 1024)


def pin(array):
    return pltpu.with_memory_space_constraint(array, pltpu.HBM)


def dot(lhs, rhs):
    return jnp.dot(lhs, rhs, preferred_element_type=F32)


def dot_t(lhs, rhs):
    return lax.dot_general(lhs, rhs, (((1,), (1,)), ((), ())), preferred_element_type=F32)


def iota(shape, dim):
    return lax.broadcasted_iota(I32, shape, dim)


def three(values):
    high = values.astype(BF16)
    rest = values - high.astype(F32)
    mid = rest.astype(BF16)
    return high, mid, (rest - mid.astype(F32)).astype(BF16)


def layer_norm(values, gain, bias):
    center = values - jnp.mean(values, -1, keepdims=True)
    spread = jnp.mean(center * center, -1, keepdims=True)
    return center * lax.rsqrt(spread + LN_EPS) * gain + bias


def route_kernel(
    me_ref,
    ids_ref,
    table_hbm,
    rows_ref,
    list_ref,
    slot_ref,
    most_ref,
    table,
    ids,
    fresh,
    chosen_ref,
    sems,
    *,
    cap,
):
    n_dest, q_dev, qlen = ids_ref.shape
    tokens = q_dev * qlen
    table_rows, width = table.shape
    parts = sems.shape[0]
    part = table_rows // parts
    copies = []
    for k in range(parts):
        piece = pl.ds(k * part, part)
        copies.append(pltpu.make_async_copy(table_hbm.at[piece], table.at[piece], sems.at[k]))
        copies[-1].start()
    for q in range(q_dev):
        ids[:, q * qlen : (q + 1) * qlen] = ids_ref[:, q, :]
    every = ids[...]
    columns = every.astype(F32).T
    earlier = iota((tokens, tokens), 0) < iota((tokens, tokens), 1)
    before = earlier.astype(F32).astype(BF16)
    for dest in range(n_dest):
        again = (columns[:, dest : dest + 1] == every[dest : dest + 1].astype(F32)) & earlier
        fresh[dest : dest + 1, :] = 1.0 - jnp.max(again.astype(F32), 0, keepdims=True)
    new = fresh[...]
    most = jnp.float32(0)
    for owner in range(n_dest):
        held = (every >= owner * table_rows) & (every < (owner + 1) * table_rows)
        most = jnp.maximum(most, jnp.max(jnp.sum(jnp.where(held, new, 0.0), -1, keepdims=True)))
    most_ref[0] = most.astype(I32)
    row = ids[pl.ds(me_ref[0], 1), :]
    at = iota(columns.shape, 1) == me_ref[0]
    column = jnp.sum(jnp.where(at, columns, 0.0), -1, keepdims=True)
    across = iota((tokens, tokens), 1).astype(F32)
    equal = column == row.astype(F32)
    first = jnp.min(jnp.where(equal, across, float(tokens)), -1, keepdims=True)
    owner = column.astype(I32) // table_rows
    same = (owner == row // table_rows) & (across < first) & (fresh[pl.ds(me_ref[0], 1), :] > 0.5)
    slot_ref[...] = owner * tokens + jnp.sum(same.astype(F32), -1, keepdims=True).astype(I32)
    offset = every - me_ref[0] * table_rows
    inside = (offset >= 0) & (offset < table_rows) & (new > 0.5)
    rank = dot(inside.astype(F32).astype(BF16), before).astype(I32)
    rank = jnp.where(inside, rank, -1)
    kept = jnp.where(inside, offset, 0)
    wide = kept.astype(F32)
    high = jnp.right_shift(kept, 7).astype(F32).astype(BF16)
    low = (kept & 127).astype(F32).astype(BF16)
    places = iota((cap, tokens), 0)
    all_places = iota((tokens, tokens), 0)
    for dest in range(n_dest):
        matches = places == rank[dest : dest + 1]
        column = jnp.sum(jnp.where(matches, wide[dest : dest + 1], 0.0), -1, keepdims=True)
        hit = iota((cap, table_rows), 1) == column.astype(I32)
        chosen_ref[dest * cap : (dest + 1) * cap, :] = hit.astype(F32).astype(BF16)
        full = (all_places == rank[dest : dest + 1]).astype(F32).astype(BF16)
        pair = jnp.concatenate([high[dest : dest + 1], low[dest : dest + 1]], 0)
        moved = dot_t(pair, full).astype(I32)
        list_ref[dest : dest + 1, :] = moved[0:1] * 128 + moved[1:2]
    for copy in copies:
        copy.wait()
    for c in range(0, width, 256):
        rows_ref[:, c : c + 256] = dot(chosen_ref[...], table[:, c : c + 256]).astype(BF16)


def route(me, all_ids, word_table, cap):
    n_dest, tokens = all_ids.shape[0], all_ids.shape[1] * all_ids.shape[2]
    table_rows, width = word_table.shape
    return pl.pallas_call(
        functools.partial(route_kernel, cap=cap),
        out_shape=(
            jax.ShapeDtypeStruct((n_dest * cap, width), BF16),
            jax.ShapeDtypeStruct((n_dest, tokens), I32),
            jax.ShapeDtypeStruct((tokens, 1), I32),
            jax.ShapeDtypeStruct((1,), I32),
        ),
        in_specs=[SM, VM, ANY],
        out_specs=(VM, VM, VM, SM),
        scratch_shapes=[
            pltpu.VMEM(word_table.shape, BF16),
            pltpu.VMEM((n_dest, tokens), I32),
            pltpu.VMEM((n_dest, tokens), F32),
            pltpu.VMEM((n_dest * cap, table_rows), BF16),
            pltpu.SemaphoreType.DMA((4 if table_rows % 64 == 0 else 1,)),
        ],
        compiler_params=grant(24),
    )(me, all_ids, word_table)


def decode_kernel(levels_ref, lengths_ref, words_ref, center_ref, docs_ref):
    many, n_words, plen = words_ref.shape
    dim = docs_ref.shape[1]
    each = dim // n_words
    spread = (iota((n_words, dim), 1) // each == iota((n_words, dim), 0)).astype(F32).astype(BF16)
    shifts = 2 * (iota((plen, dim), 1) % each)
    first = pl.program_id(0) * many
    for p in range(many):
        words = words_ref[p].astype(F32).T.astype(BF16)
        codes = jnp.right_shift(dot(words, spread).astype(I32), shifts) & 3
        residual = jnp.full(codes.shape, levels_ref[0], F32)
        for level in range(1, levels_ref.shape[0]):
            residual = jnp.where(codes == level, levels_ref[level], residual)
        summed = center_ref[p * plen : (p + 1) * plen, :].astype(F32) + residual
        unit = summed * lax.rsqrt(jnp.sum(summed * summed, -1, keepdims=True) + UNIT_EPS)
        unit = jnp.where(iota(unit.shape, 0) < lengths_ref[first + p], unit, unit[0:1])
        docs_ref[p * plen : (p + 1) * plen, :] = unit.astype(BF16)


def decode(levels, lengths, words, center):
    passages, n_words, plen = words.shape
    dim = center.shape[1]
    many = 8
    return pl.pallas_call(
        decode_kernel,
        grid=(passages // many,),
        out_shape=jax.ShapeDtypeStruct((passages * plen, dim), BF16),
        in_specs=[
            SM,
            SM,
            pl.BlockSpec((many, n_words, plen), lambda i: (i, 0, 0)),
            pl.BlockSpec((many * plen, dim), lambda i: (i, 0)),
        ],
        out_specs=pl.BlockSpec((many * plen, dim), lambda i: (i, 0)),
        compiler_params=grant(8),
    )(levels, lengths, pin(words), center)


def placed(slot_ref, recv_ref, turn, cap):
    rows, slots = slot_ref.shape[0], recv_ref.shape[0]
    owner = slot_ref[...] // rows
    rank = slot_ref[...] - owner * rows - turn * cap
    place = jnp.where((rank >= 0) & (rank < cap), owner * cap + rank, -1)
    chosen = (iota((rows, slots), 1) == place).astype(F32).astype(BF16)
    return dot(chosen, recv_ref[...])


def place_more_kernel(turn_ref, slot_ref, recv_ref, held_ref, out_ref, *, cap):
    fresh = placed(slot_ref, recv_ref, turn_ref[0], cap)
    out_ref[...] = (held_ref[...].astype(F32) + fresh).astype(BF16)


def place_more(turn, slot, recv, held, cap):
    return pl.pallas_call(
        functools.partial(place_more_kernel, cap=cap),
        out_shape=jax.ShapeDtypeStruct(held.shape, BF16),
        in_specs=[SM, VM, VM, VM],
        out_specs=VM,
        compiler_params=grant(8),
    )(turn, slot, recv, held)


def encode_kernel(
    recv_ref,
    extra_ref,
    slot_ref,
    pos_ref,
    emb_gain,
    emb_bias,
    b_qkv,
    ln1_gain,
    ln1_bias,
    b_up,
    ln2_gain,
    ln2_bias,
    w_qkv_hbm,
    w_out_hbm,
    w_up_hbm,
    w_down_hbm,
    w_proj_hbm,
    out_ref,
    w_qkv,
    w_out,
    w_up,
    w_down,
    w_proj,
    mixed_ref,
    context_ref,
    sems,
    *,
    cap,
):
    copies = []
    for source, target in (
        (w_qkv_hbm, w_qkv),
        (w_out_hbm, w_out),
        (w_up_hbm, w_up),
        (w_down_hbm, w_down),
        (w_proj_hbm, w_proj),
    ):
        part = source.shape[0] // PIECES
        copies.append([])
        for k in range(PIECES):
            cut, at = pl.ds(k * part, part), len(copies) * PIECES - PIECES + k
            copies[-1].append(pltpu.make_async_copy(source.at[cut], target.at[cut], sems.at[at]))

    def start(k):
        for copy in copies[k]:
            copy.start()

    def arrive(k):
        for copy in copies[k]:
            copy.wait()

    start(0)
    rows, width = extra_ref.shape
    qlen = pos_ref.shape[0]
    own = placed(slot_ref, recv_ref, 0, cap) + extra_ref[...].astype(F32)
    pos = pos_ref[...].astype(F32)
    embedded = own + jnp.concatenate([pos] * (rows // qlen), 0)
    hidden = layer_norm(embedded, emb_gain[...], emb_bias[...])
    arrive(0)
    for k in range(1, len(copies)):
        start(k)
    mixed_ref[...] = (dot(hidden.astype(BF16), w_qkv[...]) + b_qkv[...]).astype(BF16)
    head = width // HEADS
    per = 128 // head
    scale = head ** (-0.5)
    outside = iota((rows, rows), 0) // qlen != iota((rows, rows), 1) // qlen
    bias = jnp.where(outside, -jnp.inf, 0.0)
    lane = iota((rows, 128), 1) // head
    for i in range(width // 128):
        query = mixed_ref[:, i * 128 : (i + 1) * 128]
        keys = mixed_ref[:, width + i * 128 : width + (i + 1) * 128]
        values = mixed_ref[:, 2 * width + i * 128 : 2 * width + (i + 1) * 128]
        context = jnp.zeros((rows, 128), F32)
        for h in range(per):
            mine = lane == h
            logits = dot_t(jnp.where(mine, query, jnp.zeros_like(query)), keys) * scale + bias
            powers = jnp.exp(logits - jnp.max(logits, -1, keepdims=True))
            probs = (powers * (1.0 / jnp.sum(powers, -1, keepdims=True))).astype(BF16)
            context = context + dot(probs, jnp.where(mine, values, jnp.zeros_like(values)))
        context_ref[:, i * 128 : (i + 1) * 128] = context.astype(BF16)
    arrive(1)
    first = layer_norm(hidden + dot(context_ref[...], w_out[...]), ln1_gain[...], ln1_bias[...])
    narrow = first.astype(BF16)
    hidden_units = w_up.shape[1]
    step = width
    arrive(2)
    arrive(3)
    total = jnp.zeros((rows, width), F32)
    for c in range(hidden_units // step):
        inner = dot(narrow, w_up[:, c * step : (c + 1) * step]) + b_up[c * step : (c + 1) * step]
        inner = 0.5 * inner * (1.0 + lax.erf(inner * (0.5**0.5)))
        total = total + dot(inner.astype(BF16), w_down[c * step : (c + 1) * step, :])
    second = layer_norm(first + total, ln2_gain[...], ln2_bias[...])
    arrive(4)
    projected = dot(second.astype(BF16), w_proj[...])
    unit = projected * lax.rsqrt(jnp.sum(projected * projected, -1, keepdims=True) + UNIT_EPS)
    out_ref[...] = unit.T.astype(BF16)


def encode(recv, extra, slot, pos, vectors, weights, cap):
    rows = extra.shape[0]
    dim = weights[-1].shape[1]
    width = extra.shape[1]
    return pl.pallas_call(
        functools.partial(encode_kernel, cap=cap),
        out_shape=jax.ShapeDtypeStruct((dim, rows), BF16),
        in_specs=[VM] * (4 + len(vectors)) + [ANY] * len(weights),
        out_specs=VM,
        scratch_shapes=[pltpu.VMEM(w.shape, BF16) for w in weights]
        + [
            pltpu.VMEM((rows, 3 * width), BF16),
            pltpu.VMEM((rows, width), BF16),
            pltpu.SemaphoreType.DMA((PIECES * len(weights),)),
        ],
        compiler_params=grant(32),
    )(
        recv,
        extra,
        slot,
        pin(pos),
        *[pin(v) for v in vectors],
        *[pin(w) for w in weights],
    )


def met(place, step, half, backwards=False):
    if half & (half - 1) == 0:
        return place ^ step
    return (place + (half - step if backwards else step)) % half


def maxsim_kernel(me_ref, docs_ref, *rest, moves, partners, plen, qlen):
    query_refs = rest[: len(moves)]
    out_ref, part_ref, other_ref = rest[-3:]
    n_group, places = out_ref.shape[:2]
    many, lanes = out_ref.shape[-2:]
    half, _, rows = query_refs[0].shape
    passages = docs_ref.shape[0] // plen
    tiles = rows // 128
    segment = (iota((rows, 128), 0) // qlen == iota((rows, 128), 1)).astype(F32).astype(BF16)

    def peaks(j, part_ref):
        for b, query_ref in enumerate(query_refs):
            query = query_ref[j]
            for p in range(passages):
                sims = dot(docs_ref[p * plen : (p + 1) * plen, :], query)
                peak = jnp.max(sims.reshape(plen // 8, 8, rows), 0)
                for c in range(tiles):
                    part_ref[b * tiles + c, p * 8 : (p + 1) * 8, :] = peak[
                        :, c * 128 : (c + 1) * 128
                    ]

    def sums(j, part_ref):
        for b, (move, partner) in enumerate(zip(moves, partners)):
            bests = []
            for c in range(tiles):
                best = part_ref[b * tiles + c, pl.ds(0, passages, stride=8), :]
                for s in range(1, 8):
                    best = jnp.maximum(
                        best, part_ref[b * tiles + c, pl.ds(s, passages, stride=8), :]
                    )
                bests.append(best)
            best = jnp.concatenate(bests, 1)
            total = dot(jnp.concatenate(three(best), 0), segment)
            total = total[:passages] + (
                total[passages : 2 * passages] + total[2 * passages :]
            )
            group = lax.rem(me_ref[1] + n_group - j, n_group)
            place = met(me_ref[0] // 2, move, places, True)
            side = lax.rem(me_ref[0] + partner, 2)
            turned = total.T[:many]
            if lanes > passages:
                turned = jnp.concatenate(
                    [turned, jnp.zeros((many, lanes - passages), F32)], 1
                )
            out_ref[group, place, side] = turned

    def step(i, carry):
        peaks(2 * i, part_ref)
        sums(jnp.maximum(2 * i - 1, 0), other_ref)
        peaks(2 * i + 1, other_ref)
        sums(2 * i, part_ref)
        return carry

    if half > 1:
        lax.fori_loop(0, half // 2, step, 0)
        sums(2 * (half // 2) - 1, other_ref)
    if half % 2:
        peaks(half - 1, part_ref)
        sums(half - 1, part_ref)


def maxsim(me, docs, queries, moves, partners, previous, n_group, half, plen, qlen):
    held, dim, rows = queries[0].shape
    passages = docs.shape[0] // plen
    lanes = -(-passages // 128) * 128
    shape = (n_group, half, 2, rows // qlen, lanes)
    extra = [] if previous is None else [previous]
    many = len(queries)
    return pl.pallas_call(
        functools.partial(
            maxsim_kernel,
            moves=moves,
            partners=partners,
            plen=plen,
            qlen=qlen,
        ),
        out_shape=jax.ShapeDtypeStruct(shape, F32),
        in_specs=[SM] + [VM] * (1 + many + len(extra)),
        out_specs=VM,
        scratch_shapes=[pltpu.VMEM((many * rows // 128, passages * 8, 128), F32)] * 2,
        input_output_aliases={2 + many: 0} if extra else {},
        compiler_params=grant(8),
        cost_estimate=pl.CostEstimate(
            flops=2 * many * held * rows * docs.size, transcendentals=0, bytes_accessed=docs.size
        ),
    )(me, docs, *queries, *extra)


def select_kernel(table_ref, store_ref, local_ref, out_ref, store, local, *, passages):
    picks, q_dev, each = local_ref.shape
    rows = table_ref.shape[0]
    pairs = q_dev * each
    for q in range(q_dev):
        store[0:1, q * each : (q + 1) * each] = store_ref[q : q + 1, :] * q_dev + q
        local[:, q * each : (q + 1) * each] = local_ref[:, q, :]
    chosen = (iota((rows, pairs), 0) == store[...]).astype(F32).astype(BF16)
    high, mid, low = three(table_ref[...].T[:passages])
    own = dot(high, chosen) + (dot(mid, chosen) + dot(low, chosen))
    wanted = local[...]
    result = jnp.zeros(wanted.shape, F32)
    for p in range(passages):
        result = jnp.where(wanted == p, own[p : p + 1], result)
    for q in range(q_dev):
        out_ref[:, q, :] = result[:, q * each : (q + 1) * each]


def select(table, store, local, passages):
    picks, q_dev, each = local.shape
    return pl.pallas_call(
        functools.partial(select_kernel, passages=passages),
        out_shape=jax.ShapeDtypeStruct(local.shape, F32),
        in_specs=[VM] * 3,
        out_specs=VM,
        scratch_shapes=[pltpu.VMEM((1, q_dev * each), I32), pltpu.VMEM((picks, q_dev * each), I32)],
        compiler_params=grant(4),
    )(table, store, local)


def on_device(
    query_ids,
    word_table,
    pos_table,
    emb_gain,
    emb_bias,
    w_qkv,
    b_qkv,
    w_out,
    ln1_gain,
    ln1_bias,
    w_up,
    b_up,
    w_down,
    ln2_gain,
    ln2_bias,
    w_proj,
    centroids,
    bucket_weights,
    cand_store,
    cand_local,
    cent_ids,
    residual_words,
    lengths,
):
    n_group = lax.axis_size("group")
    n_shard = lax.axis_size("shard")
    devices = n_group * n_shard
    q_dev, qlen = query_ids.shape
    table_rows, width = word_table.shape
    rows = q_dev * qlen
    passages, plen = cent_ids.shape
    cap = -(-3 * rows // (2 * n_shard) // 16) * 16
    me = jnp.stack([lax.axis_index("shard"), lax.axis_index("group")]).astype(I32)

    all_ids = lax.all_gather(query_ids, "shard", axis=0)
    looked, asked, slot, most = route(me, all_ids, word_table, cap)

    def exchange(sent):
        sent = sent.reshape(n_shard, cap, width)
        arrived = lax.all_to_all(sent, "shard", split_axis=0, concat_axis=0, tiled=True)
        return arrived.reshape(n_shard * cap, width)

    recv = exchange(looked)

    rounds = (most[0] + cap - 1) // cap

    def more(state):
        turn, held = state
        turn, wanted, slots = lax.optimization_barrier((turn, asked, slot))
        padded = jnp.pad(wanted, ((0, 0), (0, cap)))
        offsets = lax.dynamic_slice_in_dim(padded, turn * cap, cap, 1)
        arrived = exchange(word_table[offsets.reshape(-1)])
        return turn + 1, place_more(turn.reshape(1), slots, arrived, held, cap)

    extra = lax.while_loop(
        lambda state: state[0] < rounds, more, (jnp.int32(1), jnp.zeros((rows, width), BF16))
    )[1]

    center = centroids[cent_ids.reshape(-1)]
    recv, center = lax.optimization_barrier((recv, center))
    emb = encode(
        recv,
        extra,
        slot,
        pos_table,
        (emb_gain, emb_bias, b_qkv, ln1_gain, ln1_bias, b_up, ln2_gain, ln2_bias),
        (w_qkv, w_out, w_up, w_down, w_proj),
        cap,
    )
    emb, center = lax.optimization_barrier((emb, center))

    half = n_shard // 2
    swap = [(i, i ^ 1) for i in range(n_shard)]

    def partner(block):
        return lax.ppermute(block, "shard", swap)

    def around(step):
        pairs = [(i, (i + step) % n_group) for i in range(n_group)]
        return lax.ppermute(emb, "group", pairs)

    def across(block, step):
        pairs = [(i, 2 * met(i // 2, step, half) + i % 2) for i in range(n_shard)]
        return lax.ppermute(block, "shard", pairs)

    others = [around(k) for k in range(1, n_group)]
    docs = decode(bucket_weights, lengths, residual_words, center)
    others, docs = lax.optimization_barrier((others, docs))
    column = jnp.stack([emb] + list(others))
    run = functools.partial(
        maxsim, me, docs, n_group=n_group, half=half, plen=plen, qlen=qlen
    )
    steps = [tuple(range(k, min(k + 2, half))) for k in range(1, half, 2)]
    here, sent = (column,), column
    moves = (0,)
    scores = None
    for following in steps + [()]:
        coming = tuple(across(sent, k) for k in following)
        there = tuple(partner(block) for block in here)
        if len(here) == 1 and scores is None:
            scores = run(here + there, moves * 2, (0, 1), scores)
        else:
            scores = run(here, moves, (0,) * len(here), scores)
            scores = run(there, moves, (1,) * len(here), scores)
        if following:
            coming, sent, scores = lax.optimization_barrier((coming, column, scores))
        here, moves = coming, following
    scores = scores.reshape((devices,) + scores.shape[3:])
    returned = lax.all_to_all(scores, BOTH, split_axis=0, concat_axis=0, tiled=True)
    result = select(
        returned.reshape(devices * q_dev, -1),
        cand_store,
        jnp.transpose(cand_local, (2, 0, 1)),
        passages,
    )
    return jnp.transpose(result, (1, 2, 0))


def solution(mesh):
    rows = P(BOTH)
    placed = (rows, P("shard")) + (P(),) * 16 + (rows,) * 5
    return jax.shard_map(
        on_device, mesh=mesh, in_specs=placed, out_specs=rows, check_vma=False
    )
```
